128 devices in a mesh: seq: 16 (over z_hi, x, core), chan: 8 (over z_lo, y).
Axes of the slice: x: 4, y: 4, z: 4 (z_hi: 2, z_lo: 2; z = z_hi * 2 + z_lo), core: 2. Of those that a mesh axis runs over, the one named last changes fastest.
Arguments:
- hidden_states: bfloat16 [4096, 4096], P('chan', 'seq'), may hold values from -700 to 700
- norm_gain: float32 [4096], P('chan'), may hold values from 0.1 to 1.9
- short_filter: float32 [4096, 128], P('chan'), may hold values from -0.5 to 0.5
- long_filter: bfloat16 [4096, 4096], P('chan', 'seq'), may hold values from -0.09375 to 0.09375
- long_bias: float32 [4096], P('chan'), may hold values from -4 to 4
- gate_stream: bfloat16 [4096, 4096], P('chan', 'seq'), may hold values from -6 to 6
- upstream: bfloat16 [4096, 4096], P(None, 'seq'), may hold values from -6 to 6
Outputs:
- mixed: bfloat16 [4096, 4096], P('chan', 'seq')
- weight_grad: float32 [4096, 4096], P('seq', 'chan')
The draws below stay inside these ranges and needn't reach their ends.
All inputs are finite; a program needn't handle non-finite values.
Results may differ from the reference program's by a relative error of at most 0.015.
Values may be sent and summed in bfloat16 or wider, within the bound.
No kernel may reach another device: no remote copies, remote signals or barrier semaphores. Data moves between devices by JAX's collectives and lax.ppermute only.
A program may use at most 64 MiB of HBM per device.

```python
import math
import jax
import jax.numpy as jnp
from jax import lax

D = 4096
TAPS = 128
SEQ = 4096


def draw_hidden_states(key, part):
    key_chan, key_tok, key_base = jax.random.split(jax.random.fold_in(key, 11), 3)
    channel = jnp.arange(D, dtype=jnp.float32)
    chan_scale = 3.0 ** (0.5 * channel / D) * jnp.exp(jax.random.uniform(key_chan, (D,), jnp.float32, 0.0, math.log(10.0)))
    tok_scale = jnp.exp(jax.random.uniform(key_tok, (SEQ,), jnp.float32, 0.0, math.log(10.0)))
    base = jax.random.truncated_normal(key_base, -4.0, 4.0, (D, SEQ), jnp.float32)
    return (base * chan_scale[:, None] * tok_scale[None, :]).astype(jnp.bfloat16)


def spiked(array, key, source, target, parts, factor):
    def block_of(dim):
        return (jnp.arange(array.shape[dim]) // (array.shape[dim] // parts)).reshape((-1,) + (1,) * (array.ndim - 1 - dim))

    one_side = jax.random.permutation(key, parts)[block_of(target)]
    second = (block_of(target) + parts // 2) % parts
    return jnp.where((block_of(source) == one_side) | (block_of(source) == second), factor * array, array)


def block_scale(stream_key, dims, cuts, low, largest):
    factor_of = 1.0
    for dim, parts in cuts:
        draws = jax.random.uniform(jax.random.fold_in(jax.random.fold_in(stream_key, 6), dim), (parts,), jnp.float32, low / len(cuts), largest / len(cuts))
        factor_of = factor_of * jnp.repeat(jnp.exp(draws), dims[dim] // parts).reshape((-1,) + (1,) * (len(dims) - 1 - dim))
    return factor_of


def noise(own_key, extent, deviation, limit, shards=(), kind=jnp.bfloat16):
    factor_of = block_scale(own_key, extent, shards, -0.22, 0.18) if shards else 1.0
    drawn = jax.random.normal(own_key, extent, jnp.float32) * deviation * factor_of
    return jnp.minimum(jnp.maximum(drawn, -limit), limit).astype(kind)


def noise_with(own_key, dims, scale, reach, pieces, heavy, kind=jnp.bfloat16):
    result = scale * jax.random.normal(own_key, dims, jnp.float32)
    if pieces:
        result = result * block_scale(own_key, dims, pieces, -0.22, 0.18)
    return jnp.clip(spiked(result, jax.random.fold_in(own_key, 3), *heavy), -reach, reach).astype(kind)


def setup_inputs(seed: int = 0) -> dict:
    keys = jax.random.split(jax.random.key(seed), 8)
    hidden_states = draw_hidden_states(jax.random.fold_in(keys[7], 71), 0)
    norm_gain = jnp.clip(1.0 + 0.18 * jax.random.normal(keys[1], (D,), jnp.float32), 0.1, 1.9)
    short_filter = noise(keys[2], (D, TAPS), TAPS ** -0.5, 0.5, ((0, 8),), jnp.float32)
    long_filter = noise(keys[3], (D, SEQ), SEQ ** -0.5, 0.09375, ((0, 8), (1, 16)))
    long_bias = noise(keys[4], (D,), 1.0, 4.0, ((0, 8),), jnp.float32)
    gate_stream = noise(keys[5], (D, SEQ), 1.0, 6.0, ((0, 8), (1, 16)))
    upstream = noise_with(keys[6], (D, SEQ), 1.0, 6.0, ((1, 16),), (1, 0, 16, 2.0))
    return {"hidden_states": hidden_states, "norm_gain": norm_gain, "short_filter": short_filter, "long_filter": long_filter, "long_bias": long_bias, "gate_stream": gate_stream, "upstream": upstream}


EPSILON = 1e-05

def short_conv(padded, taps):
    seq_total = padded.shape[1] - TAPS + 1

    def add_tap(index, total):
        start = (TAPS - 1 - index).astype(jnp.int32)
        window = lax.dynamic_slice_in_dim(padded, start, seq_total, 1)
        weight = lax.dynamic_slice_in_dim(taps, index.astype(jnp.int32), 1, 1)
        return total + weight * window
    initial = jnp.zeros((padded.shape[0], seq_total), jnp.float32)
    return lax.fori_loop(jnp.int32(0), jnp.int32(TAPS), add_tap, initial)

def reference(hidden_states, norm_gain, short_filter, long_filter, long_bias, gate_stream, upstream):
    states = hidden_states.astype(jnp.float32)
    squares = lax.optimization_barrier(jnp.sum(states * states, axis=0))
    normed = (states * lax.rsqrt(squares / D + EPSILON)[None, :] * norm_gain[:, None]).astype(jnp.bfloat16)
    padded = jnp.pad(normed.astype(jnp.float32), ((0, 0), (TAPS - 1, 0)))
    short_out = short_conv(padded, short_filter.astype(jnp.float32)).astype(jnp.bfloat16)
    block_width = math.gcd(D, 256)
    length = 2 * SEQ

    def one_block(pair):
        signal, filt = pair
        spec_signal = jnp.fft.rfft(signal.astype(jnp.float32), n=length, axis=1)
        spec_filter = jnp.fft.rfft(filt.astype(jnp.float32), n=length, axis=1)
        return jnp.fft.irfft(spec_signal * spec_filter, n=length, axis=1)[:, :SEQ].astype(jnp.float32)
    blocks = (short_out.reshape(D // block_width, block_width, SEQ), long_filter.reshape(D // block_width, block_width, SEQ))
    long_conv = lax.map(one_block, blocks).reshape(D, SEQ)
    long_out = (long_conv + long_bias[:, None] * short_out.astype(jnp.float32)).astype(jnp.bfloat16)
    mixed = (gate_stream.astype(jnp.float32) * long_out.astype(jnp.float32)).astype(jnp.bfloat16)
    weight_grad = lax.dot_general(upstream, mixed, (((1,), (1,)), ((), ())), preferred_element_type=jnp.float32)
    return (mixed, weight_grad)
```

```python
import functools
import math

import jax
import jax.numpy as jnp
import numpy as np
from jax import lax
from jax.experimental import pallas as pl
from jax.experimental.pallas import tpu as pltpu
from jax.sharding import PartitionSpec as P


D = 4096
EPSILON = 1e-05
OUTER = 32
INNER = 128
LENGTH = OUTER * INNER
BF16 = jnp.bfloat16
F32 = jnp.float32


def tables():
    m = np.arange(INNER, dtype=np.float64)
    turn = 2.0 * np.pi * (np.arange(OUTER)[:, None] + 0.25) * m[None, :] / LENGTH
    angle = 2.0 * np.pi * ((m[:, None] * m[None, :]) % INNER) / INNER
    cos, sin = np.cos(angle), np.sin(angle)
    ahead = np.block([[cos, -sin], [sin, cos]])
    back = np.block([[cos, sin], [-sin, cos]])
    parts = []
    for table in (ahead, back):
        upper = table.astype(BF16)
        lower = (table - upper.astype(np.float64)).astype(BF16)
        parts.append(np.concatenate([upper, lower, upper]))
    return [np.cos(turn).astype(np.float32), -np.sin(turn).astype(np.float32), *parts]


def turned(value, step, total, sign):
    re, im = value
    step %= total
    if step == 0:
        return re, im
    if 4 * step == total:
        return (-im, re) if sign > 0 else (im, -re)
    half = math.sqrt(0.5)
    if 8 * step == total:
        return ((re - im) * half, (re + im) * half) if sign > 0 else ((re + im) * half, (im - re) * half)
    if 8 * step == 3 * total:
        if sign > 0:
            return (re + im) * -half, (re - im) * half
        return (im - re) * half, (re + im) * -half
    cos = math.cos(2.0 * math.pi * step / total)
    sin = sign * math.sin(2.0 * math.pi * step / total)
    return re * cos - im * sin, re * sin + im * cos


def transform(values, sign):
    total = len(values)
    if total == 1:
        return values
    even, odd = transform(values[0::2], sign), transform(values[1::2], sign)
    first, second = [], []
    for k in range(total // 2):
        er, ei = even[k]
        dr, di = turned(odd[k], k, total, sign)
        first.append((er + dr, ei + di))
        second.append((er - dr, ei - di))
    return first + second


def in_two_passes(load, store, half_ref, sign):
    for q in range(4):
        for k, value in enumerate(transform([load(4 * p + q) for p in range(8)], sign)):
            half_ref[q, k, 0], half_ref[q, k, 1] = turned(value, q * k, OUTER, sign)
    for k in range(8):
        for j, value in enumerate(transform([(half_ref[q, k, 0], half_ref[q, k, 1]) for q in range(4)], sign)):
            store(k + 8 * j, value)


def groups_of_rows(body):
    for g in range(4):
        body(slice(8 * g, 8 * g + 8), g)


def outer_ahead(time_ref, mid_ref, half_ref, twr_ref, twi_ref):
    def group(rows, g):
        def load(n):
            x = time_ref[n, rows, :]
            angle = 2.0 * math.pi * n / (4 * OUTER)
            return x * math.cos(angle), x * -math.sin(angle)

        def store(k, value):
            re, im = value
            tr, ti = twr_ref[k : k + 1, :], twi_ref[k : k + 1, :]
            mid_ref[k, rows, 0:INNER] = re * tr - im * ti
            mid_ref[k, rows, INNER:] = re * ti + im * tr

        in_two_passes(load, store, half_ref.at[g], -1)

    groups_of_rows(group)


def outer_back(mid_ref, time_ref, half_ref, twr_ref, twi_ref):
    def group(rows, g):
        def load(k):
            re, im = mid_ref[k, rows, 0:INNER], mid_ref[k, rows, INNER:]
            tr, ti = twr_ref[k : k + 1, :], twi_ref[k : k + 1, :]
            return re * tr + im * ti, im * tr - re * ti

        def store(n, value):
            re, im = value
            angle = 2.0 * math.pi * n / (4 * OUTER)
            time_ref[n, rows, :] = re * (math.cos(angle) / LENGTH) - im * (math.sin(angle) / LENGTH)

        in_two_passes(load, store, half_ref.at[g], 1)

    groups_of_rows(group)


def product(rows, table_ref):
    upper = rows.astype(BF16)
    lower = (rows - upper.astype(F32)).astype(BF16)
    return jnp.dot(jnp.concatenate([upper, upper, lower], axis=1), table_ref[...], preferred_element_type=F32)


def complex_product(a, b):
    ar, ai, br, bi = a[:, :INNER], a[:, INNER:], b[:, :INNER], b[:, INNER:]
    return jnp.concatenate([ar * br - ai * bi, ar * bi + ai * br], axis=1)


def chunks(body):
    def step(j, carry):
        body(pl.ds(pl.multiple_of(j * 8, 8), 8))
        return carry

    lax.fori_loop(0, OUTER // 8, step, 0)


def flat(value):
    return value.reshape(value.shape[0] * value.shape[1], value.shape[2])


def column_of(row_ref, first):
    total = row_ref.shape[1]
    lane = lax.broadcasted_iota(jnp.int32, (32, total), 1)
    wanted = lax.broadcasted_iota(jnp.int32, (32, total), 0) + first
    return jnp.sum(jnp.where(lane == wanted, row_ref[...], 0.0), axis=1, keepdims=True)


def filter_kernel(got_ref, taps_ref, bias_ref, twr_ref, twi_ref, ahead, back, spec_ref, time_ref, mid_ref, half_ref):
    first = pl.multiple_of(lax.axis_index("seq") * 32, 32)
    bias = column_of(bias_ref, first)
    own_taps = taps_ref[pl.ds(first, 32), :]
    for b in range(16):
        for h in range(2):
            time_ref[2 * b + h] = got_ref[b, 32:64, h * INNER : (h + 1) * INNER].astype(F32)
    outer_ahead(time_ref, mid_ref, half_ref, twr_ref, twi_ref)

    def combine(ks):
        long = product(flat(mid_ref[ks]), ahead)
        lift = jnp.concatenate([jnp.broadcast_to(bias, (32, INNER)), jnp.zeros((32, INNER), F32)], axis=1)
        long = long + jnp.tile(lift, (8, 1))
        taps = own_taps[None]
        tr, ti = twr_ref[ks, :][:, None, :], twi_ref[ks, :][:, None, :]
        short = product(flat(jnp.concatenate([taps * tr, taps * ti], axis=2)), ahead)
        mid_ref[ks] = product(complex_product(long, short), back).reshape(8, 32, 2 * INNER)

    chunks(combine)
    outer_back(mid_ref, time_ref, half_ref, twr_ref, twi_ref)
    outer_ahead(time_ref, mid_ref, half_ref, twr_ref, twi_ref)

    def finish(ks):
        spec_ref[ks] = product(flat(mid_ref[ks]), ahead).reshape(8, 32, 2 * INNER)

    chunks(finish)


def signal_kernel(
    got_ref, squares_ref, gain_ref, spec_ref, twr_ref, twi_ref, ahead, back, mixed_ref, time_ref, mid_ref, half_ref
):
    first = lax.axis_index("seq") * 32
    gain = jnp.broadcast_to(column_of(gain_ref, first), (32, INNER))
    for b in range(16):
        scale = lax.rsqrt(jnp.sum(squares_ref[b], axis=0, keepdims=True) / D + EPSILON)
        for h in range(2):
            cols = slice(h * INNER, (h + 1) * INNER)
            normed = got_ref[b, 0:32, cols].astype(F32) * scale[:, cols] * gain
            time_ref[2 * b + h] = normed.astype(BF16).astype(F32)
    outer_ahead(time_ref, mid_ref, half_ref, twr_ref, twi_ref)

    def combine(ks):
        spec = product(flat(mid_ref[ks]), ahead)
        joint = complex_product(spec, flat(spec_ref[ks]))
        mid_ref[ks] = product(joint, back).reshape(8, 32, 2 * INNER)

    chunks(combine)
    outer_back(mid_ref, time_ref, half_ref, twr_ref, twi_ref)
    for b in range(16):
        for h in range(2):
            cols = slice(h * INNER, (h + 1) * INNER)
            long_out = time_ref[2 * b + h].astype(BF16).astype(F32)
            mixed_ref[b, :, cols] = (got_ref[b, 64:96, cols].astype(F32) * long_out).astype(BF16)


def vmem(count):
    return [pl.BlockSpec(memory_space=pltpu.VMEM)] * count


SCRATCH = [
    pltpu.VMEM((OUTER, 32, INNER), F32),
    pltpu.VMEM((OUTER, 32, 2 * INNER), F32),
    pltpu.VMEM((4, 4, 8, 2, 8, INNER), F32),
]


def filter_spectrum(got, taps, bias, consts):
    return pl.pallas_call(
        filter_kernel,
        out_shape=jax.ShapeDtypeStruct((OUTER, 32, 2 * INNER), F32),
        in_specs=vmem(7),
        out_specs=vmem(1)[0],
        scratch_shapes=SCRATCH,
        cost_estimate=pl.CostEstimate(flops=2_000_000_000, bytes_accessed=3_000_000, transcendentals=0),
        name="filter_spectrum",
    )(got, taps, bias, *consts)


def gated_convolution(got, squares, gain, spec, consts):
    return pl.pallas_call(
        signal_kernel,
        out_shape=jax.ShapeDtypeStruct((16, 32, 256), BF16),
        in_specs=vmem(8),
        out_specs=vmem(1)[0],
        scratch_shapes=SCRATCH,
        cost_estimate=pl.CostEstimate(flops=1_000_000_000, bytes_accessed=3_000_000, transcendentals=0),
    )(got, squares, gain, spec, *consts)


def pack_kernel(hidden_ref, long_ref, gate_ref, up_ref, payload_ref, squares_ref, sems):
    chan = lax.axis_index("chan")
    sources = [hidden_ref, long_ref, gate_ref, up_ref.at[:, pl.ds(pl.multiple_of(chan * 32, 32), 32), :]]
    copies = [
        pltpu.make_async_copy(source, payload_ref.at[:, 32 * i : 32 * i + 32, :], sems.at[i])
        for i, source in enumerate(sources)
    ]
    for copy in copies:
        copy.start()
    copies[0].wait()
    total = jnp.zeros((8, 256), F32)
    for b in range(16):
        states = payload_ref[b, 0:32, :].astype(F32)
        powers = states * states
        for r in range(4):
            total = total + powers[8 * r : 8 * r + 8]
    squares_ref[...] = total
    for copy in copies[1:]:
        copy.wait()


def pack(hidden, long_filter, gate, upstream):
    return pl.pallas_call(
        pack_kernel,
        out_shape=(jax.ShapeDtypeStruct((16, 128, 256), BF16), jax.ShapeDtypeStruct((8, 256), F32)),
        in_specs=[pl.BlockSpec(memory_space=pl.ANY)] * 4,
        out_specs=tuple(vmem(2)),
        scratch_shapes=[pltpu.SemaphoreType.DMA((4,))],
        name="pack",
    )(hidden, long_filter, gate, upstream)


def place_of(s):
    return s // 8, (s // 2) % 4, s % 2


def over_seq(value, dz, dx, dk):
    pairs = []
    for s in range(16):
        z, x, k = place_of(s)
        pairs.append((s, (z ^ dz) * 8 + ((x + dx) % 4) * 2 + (k ^ dk)))
    return lax.ppermute(value, "seq", pairs)


def over_chan(value, dz, dy):
    pairs = [(c, ((c // 4) ^ dz) * 4 + (c + dy) % 4) for c in range(8)]
    return lax.ppermute(value, "chan", pairs)


def around(block, move):
    right = move(block, 1)
    left = move(block, -1)
    far_a = move(right[:8], 1)
    far_b = move(left[8:], -1)
    return [(block, 0, 0), (right, 3, 0), (left, 1, 0), (far_a, 2, 0), (far_b, 2, 8)]


def gather_seq(own):
    side = over_seq(own, 1, 0, 0)
    pieces = []
    for dz, block in enumerate((own, side)):
        for value, dx, row in around(block, lambda v, d: over_seq(v, 0, d, 0)):
            pieces.append((value, 0, dz, dx, row))
            pieces.append((over_seq(value, 0, 0, 1), 1, dz, dx, row))
    return pieces


def gather_chan(own):
    side = over_chan(own, 1, 0)
    pieces = []
    for dz, block in enumerate((own, side)):
        for value, dy, row in around(block, lambda v, d: over_chan(v, 0, d)):
            pieces.append((value, dz, dy, row))
    return pieces


def whole_rows(refs, keys):
    blocks = {}
    for ref, (*key, row) in zip(refs, keys, strict=True):
        for b in range(ref.shape[0]):
            blocks.setdefault(tuple(key), {})[row + b] = (ref, b)
    values = [jnp.concatenate([rows[b][0][rows[b][1]] for b in range(16)], axis=1) for rows in blocks.values()]
    return jnp.concatenate(values, axis=0), list(blocks)


def grad_kernel(mixed_keys, up_keys, *refs):
    seq, chan = lax.axis_index("seq"), lax.axis_index("chan")
    mixed_refs, up_refs = refs[: len(mixed_keys)], refs[len(mixed_keys) : len(mixed_keys) + len(up_keys)]
    mixed_ref, grad_ref, rows_ref = refs[len(mixed_keys) + len(up_keys) :]
    mixed, sources = whole_rows(mixed_refs, mixed_keys)
    up, owners = whole_rows(up_refs, up_keys)
    total = lax.dot_general(mixed, up, (((1,), (1,)), ((), ())), preferred_element_type=F32)

    def source_place(dk, dz, dx):
        z = lax.bitwise_xor(seq // 8, dz)
        x = lax.bitwise_and(seq // 2 + dx, 3)
        k = lax.bitwise_xor(lax.bitwise_and(seq, 1), dk)
        return pl.ds(pl.multiple_of((z * 8 + x * 2 + k) * 32, 32), 32)

    for i, key in enumerate(sources):
        rows_ref[source_place(*key), :] = total[32 * i : 32 * i + 32]
    for ref, (*key, row) in zip(mixed_refs, mixed_keys, strict=True):
        place = source_place(*key)
        if ref.shape[0] == 16:
            mixed_ref[place, :] = ref[seq]
        else:

            @pl.when(seq // 8 == row // 8)
            def _(ref=ref, place=place):
                mixed_ref[place, :] = ref[lax.bitwise_and(seq, 7)]

    turned_rows = rows_ref[...].T
    for i, (dz, dy) in enumerate(owners):
        owner = lax.bitwise_xor(chan // 4, dz) * 4 + lax.bitwise_and(chan + dy, 3)
        grad_ref[pl.ds(pl.multiple_of(owner * 32, 32), 32), :] = turned_rows[32 * i : 32 * i + 32]


def weight_gradient(mixed, up):
    mixed_keys, up_keys = [piece[1:] for piece in mixed], [piece[1:] for piece in up]
    return pl.pallas_call(
        functools.partial(grad_kernel, mixed_keys, up_keys),
        out_shape=(jax.ShapeDtypeStruct((512, 256), BF16), jax.ShapeDtypeStruct((256, 512), F32)),
        in_specs=vmem(len(mixed) + len(up)),
        out_specs=tuple(vmem(2)),
        scratch_shapes=[pltpu.VMEM((512, 256), F32)],
        cost_estimate=pl.CostEstimate(flops=1_000_000_000, bytes_accessed=7_000_000, transcendentals=0),
        name="weight_gradient",
    )(*[piece[0] for piece in mixed], *[piece[0] for piece in up])


def exchange(value, axis):
    return lax.all_to_all(value, axis, split_axis=0, concat_axis=0, tiled=True)


def step(hidden_states, norm_gain, short_filter, long_filter, long_bias, gate_stream, upstream):
    consts = [jnp.asarray(table) for table in tables()]
    blocks = [value.reshape(16, 32, 256) for value in (hidden_states, long_filter, gate_stream)]
    payload, squares = pack(*blocks, upstream.reshape(16, 256, 256))
    squares = squares + over_chan(squares, 1, 0)
    got = exchange(payload, "seq")
    squares = squares + over_chan(squares, 0, 1)
    squares = squares + over_chan(squares, 0, 2)
    squares = jnp.broadcast_to(squares, (16, 8, 256))
    squares = exchange(squares, "seq")
    spec = filter_spectrum(got, short_filter, long_bias[None, :], consts)
    up = gather_chan(got[:, 96:128])
    mixed = gated_convolution(got, squares, norm_gain[None, :], spec, consts)
    return weight_gradient(gather_seq(mixed), up)


def solution(mesh):
    placed = (
        P("chan", "seq"),
        P("chan"),
        P("chan", None),
        P("chan", "seq"),
        P("chan"),
        P("chan", "seq"),
        P(None, "seq"),
    )
    return jax.shard_map(
        step,
        mesh=mesh,
        in_specs=placed,
        out_specs=(P("chan", "seq"), P("seq", "chan")),
        check_vma=False,
    )
```

```python
import functools
import math

import jax
import jax.numpy as jnp
import numpy as np
from jax import lax
from jax.experimental import pallas as pl
from jax.experimental.pallas import tpu as pltpu
from jax.sharding import PartitionSpec as P


D = 4096
EPSILON = 1e-05
OUTER = 32
INNER = 128
LENGTH = OUTER * INNER
BF16 = jnp.bfloat16
F32 = jnp.float32


def tables():
    m = np.arange(INNER, dtype=np.float64)
    turn = 2.0 * np.pi * (np.arange(OUTER)[:, None] + 0.25) * m[None, :] / LENGTH
    angle = 2.0 * np.pi * ((m[:, None] * m[None, :]) % INNER) / INNER
    cos, sin = np.cos(angle), np.sin(angle)
    ahead = np.block([[cos, -sin], [sin, cos]])
    back = np.block([[cos, sin], [-sin, cos]])
    parts = []
    for table in (ahead, back):
        upper = table.astype(BF16)
        lower = (table - upper.astype(np.float64)).astype(BF16)
        parts.append(np.concatenate([upper, lower, upper]))
    return [np.stack([np.cos(turn), -np.sin(turn)]).astype(np.float32), np.stack(parts)]


def turned(value, step, total, sign):
    re, im = value
    step %= total
    if step == 0:
        return re, im
    if 4 * step == total:
        return (-im, re) if sign > 0 else (im, -re)
    half = math.sqrt(0.5)
    if 8 * step == total:
        return ((re - im) * half, (re + im) * half) if sign > 0 else ((re + im) * half, (im - re) * half)
    if 8 * step == 3 * total:
        if sign > 0:
            return (re + im) * -half, (re - im) * half
        return (im - re) * half, (re + im) * -half
    cos = math.cos(2.0 * math.pi * step / total)
    sin = sign * math.sin(2.0 * math.pi * step / total)
    return re * cos - im * sin, re * sin + im * cos


def transform(values, sign):
    total = len(values)
    if total == 1:
        return values
    even, odd = transform(values[0::2], sign), transform(values[1::2], sign)
    first, second = [], []
    for k in range(total // 2):
        er, ei = even[k]
        dr, di = turned(odd[k], k, total, sign)
        first.append((er + dr, ei + di))
        second.append((er - dr, ei - di))
    return first + second


def in_two_passes(load, store, half_ref, sign):
    for q in range(4):
        for k, value in enumerate(transform([load(4 * p + q) for p in range(8)], sign)):
            half_ref[q, k, 0], half_ref[q, k, 1] = turned(value, q * k, OUTER, sign)
    for k in range(8):
        for j, value in enumerate(transform([(half_ref[q, k, 0], half_ref[q, k, 1]) for q in range(4)], sign)):
            store(k + 8 * j, value)


def groups_of_rows(body):
    for g in range(4):
        body(slice(8 * g, 8 * g + 8), g)


def outer_ahead(time_ref, mid_ref, half_ref, twr_ref, twi_ref):
    def group(rows, g):
        def load(n):
            x = time_ref[n, rows, :]
            angle = 2.0 * math.pi * n / (4 * OUTER)
            return x * math.cos(angle), x * -math.sin(angle)

        def store(k, value):
            re, im = value
            tr, ti = twr_ref[k : k + 1, :], twi_ref[k : k + 1, :]
            mid_ref[k, rows, 0:INNER] = re * tr - im * ti
            mid_ref[k, rows, INNER:] = re * ti + im * tr

        in_two_passes(load, store, half_ref.at[g], -1)

    groups_of_rows(group)


def outer_back(mid_ref, time_ref, half_ref, twr_ref, twi_ref):
    def group(rows, g):
        def load(k):
            re, im = mid_ref[k, rows, 0:INNER], mid_ref[k, rows, INNER:]
            tr, ti = twr_ref[k : k + 1, :], twi_ref[k : k + 1, :]
            return re * tr + im * ti, im * tr - re * ti

        def store(n, value):
            re, im = value
            angle = 2.0 * math.pi * n / (4 * OUTER)
            time_ref[n, rows, :] = re * (math.cos(angle) / LENGTH) - im * (math.sin(angle) / LENGTH)

        in_two_passes(load, store, half_ref.at[g], 1)

    groups_of_rows(group)


def product(rows, table_ref):
    upper = rows.astype(BF16)
    lower = (rows - upper.astype(F32)).astype(BF16)
    return jnp.dot(jnp.concatenate([upper, upper, lower], axis=1), table_ref[...], preferred_element_type=F32)


def complex_product(a, b):
    ar, ai, br, bi = a[:, :INNER], a[:, INNER:], b[:, :INNER], b[:, INNER:]
    return jnp.concatenate([ar * br - ai * bi, ar * bi + ai * br], axis=1)


def chunks(body):
    def step(j, carry):
        body(pl.ds(pl.multiple_of(j * 8, 8), 8))
        return carry

    lax.fori_loop(0, OUTER // 8, step, 0)


def flat(value):
    return value.reshape(value.shape[0] * value.shape[1], value.shape[2])


def column_of(row_ref, first):
    total = row_ref.shape[1]
    lane = lax.broadcasted_iota(jnp.int32, (32, total), 1)
    wanted = lax.broadcasted_iota(jnp.int32, (32, total), 0) + first
    return jnp.sum(jnp.where(lane == wanted, row_ref[...], 0.0), axis=1, keepdims=True)


def filter_kernel(
    got_ref, taps_ref, bias_ref, turn_hbm, inner_hbm, spec_ref, time_ref, mid_ref, half_ref, turn_ref, inner_ref, sems
):
    turn_copy, inner_copy = fetch((turn_hbm, inner_hbm), (turn_ref, inner_ref), sems)
    twr_ref, twi_ref, ahead, back = turn_ref.at[0], turn_ref.at[1], inner_ref.at[0], inner_ref.at[1]
    first = pl.multiple_of(lax.axis_index("seq") * 32, 32)
    bias = column_of(bias_ref, first)
    own_taps = taps_ref[pl.ds(first, 32), :]
    for b in range(16):
        for h in range(2):
            time_ref[2 * b + h] = got_ref[b, 0:32, h * INNER : (h + 1) * INNER].astype(F32)
    turn_copy.wait()
    outer_ahead(time_ref, mid_ref, half_ref, twr_ref, twi_ref)
    inner_copy.wait()

    def combine(ks):
        long = product(flat(mid_ref[ks]), ahead)
        lift = jnp.concatenate([jnp.broadcast_to(bias, (32, INNER)), jnp.zeros((32, INNER), F32)], axis=1)
        long = long + jnp.tile(lift, (8, 1))
        taps = own_taps[None]
        tr, ti = twr_ref[ks, :][:, None, :], twi_ref[ks, :][:, None, :]
        short = product(flat(jnp.concatenate([taps * tr, taps * ti], axis=2)), ahead)
        mid_ref[ks] = product(complex_product(long, short), back).reshape(8, 32, 2 * INNER)

    chunks(combine)
    outer_back(mid_ref, time_ref, half_ref, twr_ref, twi_ref)
    outer_ahead(time_ref, mid_ref, half_ref, twr_ref, twi_ref)

    def finish(ks):
        spec_ref[ks] = product(flat(mid_ref[ks]), ahead).reshape(8, 32, 2 * INNER)

    chunks(finish)


def signal_kernel(
    normed_ref,
    got_ref,
    spec_any,
    turn_hbm,
    inner_hbm,
    mixed_ref,
    time_ref,
    mid_ref,
    half_ref,
    turn_ref,
    inner_ref,
    sems,
    spec_ref,
):
    copies = fetch((turn_hbm, inner_hbm, spec_any), (turn_ref, inner_ref, spec_ref), sems)
    twr_ref, twi_ref, ahead, back = turn_ref.at[0], turn_ref.at[1], inner_ref.at[0], inner_ref.at[1]
    for b in range(16):
        for h in range(2):
            time_ref[2 * b + h] = normed_ref[b, :, h * INNER : (h + 1) * INNER].astype(F32)
    copies[0].wait()
    outer_ahead(time_ref, mid_ref, half_ref, twr_ref, twi_ref)
    copies[1].wait()
    copies[2].wait()

    def combine(ks):
        spec = product(flat(mid_ref[ks]), ahead)
        joint = complex_product(spec, flat(spec_ref[ks]))
        mid_ref[ks] = product(joint, back).reshape(8, 32, 2 * INNER)

    chunks(combine)
    outer_back(mid_ref, time_ref, half_ref, twr_ref, twi_ref)
    for b in range(16):
        for h in range(2):
            cols = slice(h * INNER, (h + 1) * INNER)
            long_out = time_ref[2 * b + h].astype(BF16).astype(F32)
            mixed_ref[b, :, cols] = (got_ref[b, 32:64, cols].astype(F32) * long_out).astype(BF16)


def vmem(count):
    return [pl.BlockSpec(memory_space=pltpu.VMEM)] * count


def hbm(count):
    return [pl.BlockSpec(memory_space=pltpu.HBM)] * count


def stay(value):
    return pltpu.with_memory_space_constraint(value, pltpu.HBM)


def fetch(sources, targets, sems):
    copies = [pltpu.make_async_copy(source, target, sems.at[i]) for i, (source, target) in enumerate(zip(sources, targets))]
    for copy in copies:
        copy.start()
    return copies


SCRATCH = [
    pltpu.VMEM((OUTER, 32, INNER), F32),
    pltpu.VMEM((OUTER, 32, 2 * INNER), F32),
    pltpu.VMEM((4, 4, 8, 2, 8, INNER), F32),
    pltpu.VMEM((2, OUTER, INNER), F32),
    pltpu.VMEM((2, 6 * INNER, 2 * INNER), BF16),
    pltpu.SemaphoreType.DMA((3,)),
]


def filter_spectrum(got, taps, bias, consts):
    return pl.pallas_call(
        filter_kernel,
        out_shape=jax.ShapeDtypeStruct((OUTER, 32, 2 * INNER), F32),
        in_specs=vmem(3) + hbm(2),
        out_specs=vmem(1)[0],
        scratch_shapes=SCRATCH,
        cost_estimate=pl.CostEstimate(flops=2_000_000_000, bytes_accessed=3_000_000, transcendentals=0),
        compiler_params=limit(8),
        name="filter_spectrum",
    )(got, taps, bias, *[stay(value) for value in consts])


def gated_convolution(normed, got, spec, consts):
    return pl.pallas_call(
        signal_kernel,
        out_shape=jax.ShapeDtypeStruct((16, 32, 256), BF16),
        in_specs=[*vmem(2), pl.BlockSpec(memory_space=pl.ANY), *hbm(2)],
        out_specs=vmem(1)[0],
        scratch_shapes=[*SCRATCH, pltpu.VMEM((OUTER, 32, 2 * INNER), F32)],
        cost_estimate=pl.CostEstimate(flops=1_000_000_000, bytes_accessed=3_000_000, transcendentals=0),
        compiler_params=limit(8),
    )(normed, got, stay(spec), *[stay(value) for value in consts])


def pack_kernel(hidden_ref, long_ref, gate_ref, up_ref, payload_ref, squares_ref, hidden, sems):
    chan = lax.axis_index("chan")
    sources = [long_ref, gate_ref, up_ref.at[:, pl.ds(pl.multiple_of(chan * 32, 32), 32), :]]
    copies = [pltpu.make_async_copy(hidden_ref, hidden, sems.at[3])]
    for i, source in enumerate(sources):
        copies.append(pltpu.make_async_copy(source, payload_ref.at[:, 32 * i : 32 * i + 32, :], sems.at[i]))
    for copy in copies:
        copy.start()
    copies[0].wait()
    total = jnp.zeros((8, 256), F32)
    for b in range(16):
        states = hidden[b].astype(F32)
        powers = states * states
        for r in range(4):
            total = total + powers[8 * r : 8 * r + 8]
    squares_ref[...] = total
    for copy in copies[1:]:
        copy.wait()


def limit(mib):
    return pltpu.CompilerParams(vmem_limit_bytes=mib * 2**20)


def pack(hidden, long_filter, gate, upstream):
    return pl.pallas_call(
        pack_kernel,
        out_shape=(jax.ShapeDtypeStruct((16, 96, 256), BF16), jax.ShapeDtypeStruct((8, 256), F32)),
        in_specs=hbm(4),
        out_specs=tuple(vmem(2)),
        scratch_shapes=[pltpu.VMEM((16, 32, 256), BF16), pltpu.SemaphoreType.DMA((4,))],
        compiler_params=limit(6),
        name="pack",
    )(*[stay(value) for value in (hidden, long_filter, gate, upstream)])


def place_of(s):
    return s // 8, (s // 2) % 4, s % 2


def over_seq(value, dz, dx, dk):
    pairs = []
    for s in range(16):
        z, x, k = place_of(s)
        pairs.append((s, (z ^ dz) * 8 + ((x + dx) % 4) * 2 + (k ^ dk)))
    return lax.ppermute(value, "seq", pairs)


def over_chan(value, dz, dy):
    pairs = [(c, ((c // 4) ^ dz) * 4 + (c + dy) % 4) for c in range(8)]
    return lax.ppermute(value, "chan", pairs)


def gather_seq(own):
    side = over_seq(own, 1, 0, 0)
    near = {(0, 0): own, (1, 0): side}
    for dx in (3, 1, 2):
        near[0, dx] = over_seq(own, 0, -dx, 0)
    for dx in (3, 1):
        near[1, dx] = over_seq(side, 0, -dx, 0)
    near[1, 2] = over_seq(near[0, 2], 1, 0, 0)
    pieces = []
    for (dz, dx), value in near.items():
        pieces += [(value, 0, dz, dx), (over_seq(value, 0, 0, 1), 1, dz, dx)]
    return pieces


def gather_chan(own):
    side = over_chan(own, 1, 0)
    pieces = [(own, 0, 0), (side, 1, 0)]
    for dz, block in enumerate((own, side)):
        for dy in (3, 1, 2):
            pieces.append((over_chan(block, 0, -dy), dz, dy))
    return pieces


def whole_rows(refs):
    return jnp.concatenate([jnp.concatenate([ref[b] for b in range(16)], axis=1) for ref in refs], axis=0)


def grad_kernel(mixed_keys, up_keys, *refs):
    seq, chan = lax.axis_index("seq"), lax.axis_index("chan")
    mixed_refs, up_refs = refs[: len(mixed_keys)], refs[len(mixed_keys) : len(mixed_keys) + len(up_keys)]
    mixed_ref, grad_ref, rows_ref = refs[len(mixed_keys) + len(up_keys) :]
    total = lax.dot_general(whole_rows(mixed_refs), whole_rows(up_refs), (((1,), (1,)), ((), ())), preferred_element_type=F32)

    def source_place(dk, dz, dx):
        z = lax.bitwise_xor(seq // 8, dz)
        x = lax.bitwise_and(seq // 2 + dx, 3)
        k = lax.bitwise_xor(lax.bitwise_and(seq, 1), dk)
        return pl.ds(pl.multiple_of((z * 8 + x * 2 + k) * 32, 32), 32)

    for i, (ref, key) in enumerate(zip(mixed_refs, mixed_keys, strict=True)):
        place = source_place(*key)
        rows_ref[place, :] = total[32 * i : 32 * i + 32]
        mixed_ref[place, :] = ref[seq]
    turned_rows = rows_ref[...].T
    for i, (dz, dy) in enumerate(up_keys):
        owner = lax.bitwise_xor(chan // 4, dz) * 4 + lax.bitwise_and(chan + dy, 3)
        grad_ref[pl.ds(pl.multiple_of(owner * 32, 32), 32), :] = turned_rows[32 * i : 32 * i + 32]


def weight_gradient(mixed, up):
    mixed_keys, up_keys = [piece[1:] for piece in mixed], [piece[1:] for piece in up]
    return pl.pallas_call(
        functools.partial(grad_kernel, mixed_keys, up_keys),
        out_shape=(jax.ShapeDtypeStruct((512, 256), BF16), jax.ShapeDtypeStruct((256, 512), F32)),
        in_specs=vmem(len(mixed) + len(up)),
        out_specs=tuple(vmem(2)),
        scratch_shapes=[pltpu.VMEM((512, 256), F32)],
        cost_estimate=pl.CostEstimate(flops=1_000_000_000, bytes_accessed=7_000_000, transcendentals=0),
        compiler_params=limit(16),
        name="weight_gradient",
    )(*[piece[0] for piece in mixed], *[piece[0] for piece in up])


def exchange(value, axis):
    return lax.all_to_all(value, axis, split_axis=0, concat_axis=0, tiled=True)


def step(hidden_states, norm_gain, short_filter, long_filter, long_bias, gate_stream, upstream):
    consts = [jnp.asarray(table) for table in tables()]
    blocks = [value.reshape(16, 32, 256) for value in (hidden_states, long_filter, gate_stream)]
    payload, squares = pack(*blocks, upstream.reshape(16, 256, 256))
    squares = squares + over_chan(squares, 1, 0)
    got = exchange(payload, "seq")
    squares = squares + over_chan(squares, 0, 1)
    squares = squares + over_chan(squares, 0, 2)
    scale = lax.rsqrt(jnp.sum(squares, axis=0) / D + EPSILON)
    normed = (hidden_states.astype(F32) * scale[None, :] * norm_gain[:, None]).astype(BF16)
    normed = exchange(normed.reshape(16, 32, 256), "seq")
    spec = filter_spectrum(got, short_filter, long_bias[None, :], consts)
    up = gather_chan(got[:, 64:96])
    mixed = gated_convolution(normed, got, spec, consts)
    return weight_gradient(gather_seq(mixed), up)


def solution(mesh):
    placed = (
        P("chan", "seq"),
        P("chan"),
        P("chan", None),
        P("chan", "seq"),
        P("chan"),
        P("chan", "seq"),
        P(None, "seq"),
    )
    return jax.shard_map(
        step,
        mesh=mesh,
        in_specs=placed,
        out_specs=(P("chan", "seq"), P("seq", "chan")),
        check_vma=False,
    )
```

```python
import functools
import math

import jax
import jax.numpy as jnp
import numpy as np
from jax import lax
from jax.experimental import pallas as pl
from jax.experimental.pallas import tpu as pltpu
from jax.sharding import PartitionSpec as P


D = 4096
EPSILON = 1e-05
OUTER = 32
INNER = 128
LENGTH = OUTER * INNER
BF16 = jnp.bfloat16
F32 = jnp.float32


def tables():
    m = np.arange(INNER, dtype=np.float64)
    turn = 2.0 * np.pi * (np.arange(OUTER)[:, None] + 0.25) * m[None, :] / LENGTH
    angle = 2.0 * np.pi * ((m[:, None] * m[None, :]) % INNER) / INNER
    cos, sin = np.cos(angle), np.sin(angle)
    ahead = np.block([[cos, -sin], [sin, cos]])
    back = np.block([[cos, sin], [-sin, cos]])
    parts = []
    for table in (ahead, back):
        upper = table.astype(BF16)
        lower = (table - upper.astype(np.float64)).astype(BF16)
        parts.append(np.concatenate([upper, lower, upper]))
    return [np.stack([np.cos(turn), -np.sin(turn)]).astype(np.float32), np.stack(parts)]


def turned(value, step, total, sign):
    re, im = value
    step %= total
    if step == 0:
        return re, im
    if 4 * step == total:
        return (-im, re) if sign > 0 else (im, -re)
    half = math.sqrt(0.5)
    if 8 * step == total:
        return ((re - im) * half, (re + im) * half) if sign > 0 else ((re + im) * half, (im - re) * half)
    if 8 * step == 3 * total:
        if sign > 0:
            return (re + im) * -half, (re - im) * half
        return (im - re) * half, (re + im) * -half
    cos = math.cos(2.0 * math.pi * step / total)
    sin = sign * math.sin(2.0 * math.pi * step / total)
    return re * cos - im * sin, re * sin + im * cos


def transform(values, sign):
    total = len(values)
    if total == 1:
        return values
    even, odd = transform(values[0::2], sign), transform(values[1::2], sign)
    first, second = [], []
    for k in range(total // 2):
        er, ei = even[k]
        dr, di = turned(odd[k], k, total, sign)
        first.append((er + dr, ei + di))
        second.append((er - dr, ei - di))
    return first + second


def in_two_passes(load, store, half_ref, sign):
    for q in range(4):
        for k, value in enumerate(transform([load(4 * p + q) for p in range(8)], sign)):
            half_ref[q, k, 0], half_ref[q, k, 1] = turned(value, q * k, OUTER, sign)
    for k in range(8):
        for j, value in enumerate(transform([(half_ref[q, k, 0], half_ref[q, k, 1]) for q in range(4)], sign)):
            store(k + 8 * j, value)


def groups_of_rows(body):
    for g in range(4):
        body(slice(8 * g, 8 * g + 8), g)


def outer_ahead(time_ref, mid_ref, half_ref, twr_ref, twi_ref):
    def group(rows, g):
        def load(n):
            x = time_ref[n, rows, :]
            angle = 2.0 * math.pi * n / (4 * OUTER)
            return x * math.cos(angle), x * -math.sin(angle)

        def store(k, value):
            re, im = value
            tr, ti = twr_ref[k : k + 1, :], twi_ref[k : k + 1, :]
            mid_ref[k, rows, 0:INNER] = re * tr - im * ti
            mid_ref[k, rows, INNER:] = re * ti + im * tr

        in_two_passes(load, store, half_ref.at[g], -1)

    groups_of_rows(group)


def outer_back(mid_ref, time_ref, half_ref, twr_ref, twi_ref):
    def group(rows, g):
        def load(k):
            re, im = mid_ref[k, rows, 0:INNER], mid_ref[k, rows, INNER:]
            tr, ti = twr_ref[k : k + 1, :], twi_ref[k : k + 1, :]
            return re * tr + im * ti, im * tr - re * ti

        def store(n, value):
            re, im = value
            angle = 2.0 * math.pi * n / (4 * OUTER)
            time_ref[n, rows, :] = re * (math.cos(angle) / LENGTH) - im * (math.sin(angle) / LENGTH)

        in_two_passes(load, store, half_ref.at[g], 1)

    groups_of_rows(group)


def product(rows, table_ref):
    upper = rows.astype(BF16)
    lower = (rows - upper.astype(F32)).astype(BF16)
    return jnp.dot(jnp.concatenate([upper, upper, lower], axis=1), table_ref[...], preferred_element_type=F32)


def complex_product(a, b):
    ar, ai, br, bi = a[:, :INNER], a[:, INNER:], b[:, :INNER], b[:, INNER:]
    return jnp.concatenate([ar * br - ai * bi, ar * bi + ai * br], axis=1)


def chunks(body):
    def step(j, carry):
        body(pl.ds(pl.multiple_of(j * 8, 8), 8))
        return carry

    lax.fori_loop(0, OUTER // 8, step, 0)


def flat(value):
    return value.reshape(value.shape[0] * value.shape[1], value.shape[2])


def column_of(row_ref, first):
    total = row_ref.shape[1]
    lane = lax.broadcasted_iota(jnp.int32, (32, total), 1)
    wanted = lax.broadcasted_iota(jnp.int32, (32, total), 0) + first
    return jnp.sum(jnp.where(lane == wanted, row_ref[...], 0.0), axis=1, keepdims=True)


def filter_kernel(
    got_ref,
    taps_ref,
    bias_ref,
    turn_hbm,
    inner_hbm,
    spec_hbm,
    time_ref,
    mid_ref,
    half_ref,
    turn_ref,
    inner_ref,
    sems,
    spec_ref,
    out_sems,
):
    turn_copy, inner_copy = fetch((turn_hbm, inner_hbm), (turn_ref, inner_ref), sems)
    twr_ref, twi_ref, ahead, back = turn_ref.at[0], turn_ref.at[1], inner_ref.at[0], inner_ref.at[1]
    first = pl.multiple_of(lax.axis_index("seq") * 32, 32)
    bias = column_of(bias_ref, first)
    own_taps = taps_ref[pl.ds(first, 32), :]
    for b in range(16):
        for h in range(2):
            time_ref[2 * b + h] = got_ref[b, 0:32, h * INNER : (h + 1) * INNER].astype(F32)
    turn_copy.wait()
    outer_ahead(time_ref, mid_ref, half_ref, twr_ref, twi_ref)
    inner_copy.wait()

    def combine(ks):
        long = product(flat(mid_ref[ks]), ahead)
        lift = jnp.concatenate([jnp.broadcast_to(bias, (32, INNER)), jnp.zeros((32, INNER), F32)], axis=1)
        long = long + jnp.tile(lift, (8, 1))
        taps = own_taps[None]
        tr, ti = twr_ref[ks, :][:, None, :], twi_ref[ks, :][:, None, :]
        short = product(flat(jnp.concatenate([taps * tr, taps * ti], axis=2)), ahead)
        mid_ref[ks] = product(complex_product(long, short), back).reshape(8, 32, 2 * INNER)

    chunks(combine)
    outer_back(mid_ref, time_ref, half_ref, twr_ref, twi_ref)
    outer_ahead(time_ref, mid_ref, half_ref, twr_ref, twi_ref)

    copies = []
    for j in range(OUTER // 8):
        ks = slice(8 * j, 8 * j + 8)
        spec_ref[ks] = product(flat(mid_ref[ks]), ahead).reshape(8, 32, 2 * INNER)
        copies.append(pltpu.make_async_copy(spec_ref.at[ks], spec_hbm.at[ks], out_sems.at[j]))
        copies[-1].start()
    for copy in copies:
        copy.wait()


def signal_kernel(
    got_ref, spec_hbm, turn_hbm, inner_hbm, mixed_ref, time_ref, mid_ref, half_ref, turn_ref, inner_ref, sems, spec_ref
):
    copies = fetch((turn_hbm, inner_hbm, spec_hbm), (turn_ref, inner_ref, spec_ref), sems)
    twr_ref, twi_ref, ahead, back = turn_ref.at[0], turn_ref.at[1], inner_ref.at[0], inner_ref.at[1]
    for b in range(16):
        for h in range(2):
            time_ref[2 * b + h] = got_ref[b, 0:32, h * INNER : (h + 1) * INNER].astype(F32)
    copies[0].wait()
    outer_ahead(time_ref, mid_ref, half_ref, twr_ref, twi_ref)
    copies[1].wait()
    copies[2].wait()

    def combine(ks):
        spec = product(flat(mid_ref[ks]), ahead)
        joint = complex_product(spec, flat(spec_ref[ks]))
        mid_ref[ks] = product(joint, back).reshape(8, 32, 2 * INNER)

    chunks(combine)
    outer_back(mid_ref, time_ref, half_ref, twr_ref, twi_ref)
    for b in range(16):
        for h in range(2):
            cols = slice(h * INNER, (h + 1) * INNER)
            long_out = time_ref[2 * b + h].astype(BF16).astype(F32)
            mixed_ref[b, :, cols] = (got_ref[b, 32:64, cols].astype(F32) * long_out).astype(BF16)


def vmem(count):
    return [pl.BlockSpec(memory_space=pltpu.VMEM)] * count


def hbm(count):
    return [pl.BlockSpec(memory_space=pltpu.HBM)] * count


def stay(value):
    return pltpu.with_memory_space_constraint(value, pltpu.HBM)


def fetch(sources, targets, sems):
    copies = [pltpu.make_async_copy(source, target, sems.at[i]) for i, (source, target) in enumerate(zip(sources, targets))]
    for copy in copies:
        copy.start()
    return copies


SCRATCH = [
    pltpu.VMEM((OUTER, 32, INNER), F32),
    pltpu.VMEM((OUTER, 32, 2 * INNER), F32),
    pltpu.VMEM((4, 4, 8, 2, 8, INNER), F32),
    pltpu.VMEM((2, OUTER, INNER), F32),
    pltpu.VMEM((2, 6 * INNER, 2 * INNER), BF16),
    pltpu.SemaphoreType.DMA((3,)),
]


def filter_spectrum(got, taps, bias, consts):
    return pl.pallas_call(
        filter_kernel,
        out_shape=pltpu.HBM((OUTER, 32, 2 * INNER), F32),
        in_specs=vmem(3) + hbm(2),
        out_specs=hbm(1)[0],
        scratch_shapes=[*SCRATCH, pltpu.VMEM((OUTER, 32, 2 * INNER), F32), pltpu.SemaphoreType.DMA((4,))],
        cost_estimate=pl.CostEstimate(flops=2_000_000_000, bytes_accessed=3_000_000, transcendentals=0),
        compiler_params=limit(8),
        name="filter_spectrum",
    )(got, taps, bias, *[stay(value) for value in consts])


def gated_convolution(got, spec, consts):
    return pl.pallas_call(
        signal_kernel,
        out_shape=jax.ShapeDtypeStruct((16, 32, 256), BF16),
        in_specs=vmem(1) + hbm(3),
        out_specs=vmem(1)[0],
        scratch_shapes=[*SCRATCH, pltpu.VMEM((OUTER, 32, 2 * INNER), F32)],
        cost_estimate=pl.CostEstimate(flops=1_000_000_000, bytes_accessed=3_000_000, transcendentals=0),
        compiler_params=limit(8),
    )(got, stay(spec), *[stay(value) for value in consts])


def pack_kernel(hidden_hbm, long_ref, up_ref, gain_hbm, payload_ref, squares_ref, lifted_ref, hidden, gain_ref, sems):
    chan = lax.axis_index("chan")
    own_up = up_ref.at[:, pl.ds(pl.multiple_of(chan * 32, 32), 32), :]
    targets = [gain_ref, hidden, payload_ref.at[:, 0:32, :], payload_ref.at[:, 32:64, :]]
    copies = fetch([gain_hbm, hidden_hbm, long_ref, own_up], targets, sems)
    copies[0].wait()
    gains = [jnp.broadcast_to(gain_ref[q : q + 1, :], (INNER, INNER)).T for q in range(4)]
    copies[1].wait()
    total = jnp.zeros((8, 256), F32)
    for b in range(16):
        states = hidden[b].astype(F32)
        powers = states * states
        for r in range(4):
            total = total + powers[8 * r : 8 * r + 8]
        gain = gains[b // 4][32 * (b % 4) : 32 * (b % 4) + 32]
        lifted_ref[b] = states * jnp.concatenate([gain, gain], axis=1)
    squares_ref[...] = total
    for copy in copies[2:]:
        copy.wait()


def norm_kernel(lifted_ref, s0, s1, s2, s3, gate_hbm, payload_ref, sems):
    (copy,) = fetch([gate_hbm], [payload_ref.at[:, 32:64, :]], sems)
    squares = (s0[...] + s1[...]) + (s2[...] + s3[...])
    scale = lax.rsqrt(jnp.sum(squares, axis=0, keepdims=True) / D + EPSILON)
    for b in range(16):
        payload_ref[b, 0:32, :] = (lifted_ref[b] * scale).astype(BF16)
    copy.wait()


def limit(mib):
    return pltpu.CompilerParams(vmem_limit_bytes=mib * 2**20)


def pack(hidden, long_filter, upstream, gain):
    return pl.pallas_call(
        pack_kernel,
        out_shape=(
            jax.ShapeDtypeStruct((16, 64, 256), BF16),
            jax.ShapeDtypeStruct((8, 256), F32),
            jax.ShapeDtypeStruct((16, 32, 256), F32),
        ),
        in_specs=hbm(4),
        out_specs=tuple(vmem(3)),
        scratch_shapes=[
            pltpu.VMEM((16, 32, 256), BF16),
            pltpu.VMEM((4, INNER), F32),
            pltpu.SemaphoreType.DMA((4,)),
        ],
        compiler_params=limit(6),
        name="pack",
    )(stay(hidden), stay(long_filter), stay(upstream), stay(gain))


def normalise(lifted, squares, gate):
    return pl.pallas_call(
        norm_kernel,
        out_shape=jax.ShapeDtypeStruct((16, 64, 256), BF16),
        in_specs=vmem(5) + hbm(1),
        out_specs=vmem(1)[0],
        scratch_shapes=[pltpu.SemaphoreType.DMA((1,))],
        compiler_params=limit(6),
        name="normalise",
    )(lifted, *squares, stay(gate))


def place_of(s):
    return s // 8, (s // 2) % 4, s % 2


def over_seq(value, dz, dx, dk):
    pairs = []
    for s in range(16):
        z, x, k = place_of(s)
        pairs.append((s, (z ^ dz) * 8 + ((x + dx) % 4) * 2 + (k ^ dk)))
    return lax.ppermute(value, "seq", pairs)


def over_chan(value, dz, dy):
    pairs = [(c, ((c // 4) ^ dz) * 4 + (c + dy) % 4) for c in range(8)]
    return lax.ppermute(value, "chan", pairs)


def gather_seq(own):
    side = over_seq(own, 1, 0, 0)
    near = {(0, 0): own, (1, 0): side}
    for dx in (3, 1, 2):
        near[0, dx] = over_seq(own, 0, -dx, 0)
    for dx in (3, 1):
        near[1, dx] = over_seq(side, 0, -dx, 0)
    near[1, 2] = over_seq(near[0, 2], 1, 0, 0)
    pieces = []
    for (dz, dx), value in near.items():
        pieces += [(value, 0, dz, dx), (over_seq(value, 0, 0, 1), 1, dz, dx)]
    return pieces


def gather_chan(own):
    side = over_chan(own, 1, 0)
    pieces = [(own, 0, 0), (side, 1, 0)]
    for dz, block in enumerate((own, side)):
        for dy in (3, 1, 2):
            pieces.append((over_chan(block, 0, -dy), dz, dy))
    return pieces


def whole_rows(refs):
    return jnp.concatenate([jnp.concatenate([ref[b] for b in range(16)], axis=1) for ref in refs], axis=0)


def grad_kernel(mixed_keys, up_keys, *refs):
    seq, chan = lax.axis_index("seq"), lax.axis_index("chan")
    mixed_refs, up_refs = refs[: len(mixed_keys)], refs[len(mixed_keys) : len(mixed_keys) + len(up_keys)]
    mixed_ref, grad_ref, rows_ref = refs[len(mixed_keys) + len(up_keys) :]
    total = lax.dot_general(whole_rows(mixed_refs), whole_rows(up_refs), (((1,), (1,)), ((), ())), preferred_element_type=F32)

    def source_place(dk, dz, dx):
        z = lax.bitwise_xor(seq // 8, dz)
        x = lax.bitwise_and(seq // 2 + dx, 3)
        k = lax.bitwise_xor(lax.bitwise_and(seq, 1), dk)
        return pl.ds(pl.multiple_of((z * 8 + x * 2 + k) * 32, 32), 32)

    for i, (ref, key) in enumerate(zip(mixed_refs, mixed_keys, strict=True)):
        place = source_place(*key)
        rows_ref[place, :] = total[32 * i : 32 * i + 32]
        mixed_ref[place, :] = ref[seq]
    turned_rows = rows_ref[...].T
    for i, (dz, dy) in enumerate(up_keys):
        owner = lax.bitwise_xor(chan // 4, dz) * 4 + lax.bitwise_and(chan + dy, 3)
        grad_ref[pl.ds(pl.multiple_of(owner * 32, 32), 32), :] = turned_rows[32 * i : 32 * i + 32]


def weight_gradient(mixed, up):
    mixed_keys, up_keys = [piece[1:] for piece in mixed], [piece[1:] for piece in up]
    return pl.pallas_call(
        functools.partial(grad_kernel, mixed_keys, up_keys),
        out_shape=(jax.ShapeDtypeStruct((512, 256), BF16), jax.ShapeDtypeStruct((256, 512), F32)),
        in_specs=vmem(len(mixed) + len(up)),
        out_specs=tuple(vmem(2)),
        scratch_shapes=[pltpu.VMEM((512, 256), F32)],
        cost_estimate=pl.CostEstimate(flops=1_000_000_000, bytes_accessed=7_000_000, transcendentals=0),
        compiler_params=limit(16),
        name="weight_gradient",
    )(*[piece[0] for piece in mixed], *[piece[0] for piece in up])


def exchange(value, axis):
    return lax.all_to_all(value, axis, split_axis=0, concat_axis=0, tiled=True)


def step(hidden_states, norm_gain, short_filter, long_filter, long_bias, gate_stream, upstream):
    consts = [jnp.asarray(table) for table in tables()]
    hidden, filt, gate = [value.reshape(16, 32, 256) for value in (hidden_states, long_filter, gate_stream)]
    payload, squares, lifted = pack(hidden, filt, upstream.reshape(16, 256, 256), norm_gain.reshape(4, INNER))
    squares = squares + over_chan(squares, 1, 0)
    got = exchange(payload, "seq")
    parts = [squares]
    for dy in (1, 3, 2):
        parts.append(over_chan(squares, 0, dy))
    payload = normalise(lifted, parts, gate)
    signal = exchange(payload, "seq")
    spec = filter_spectrum(got, short_filter, long_bias[None, :], consts)
    up = gather_chan(got[:, 32:64])
    mixed = gated_convolution(signal, spec, consts)
    return weight_gradient(gather_seq(mixed), up)


def solution(mesh):
    placed = (
        P("chan", "seq"),
        P("chan"),
        P("chan", None),
        P("chan", "seq"),
        P("chan"),
        P("chan", "seq"),
        P(None, "seq"),
    )
    return jax.shard_map(
        step,
        mesh=mesh,
        in_specs=placed,
        out_specs=(P("chan", "seq"), P("seq", "chan")),
        check_vma=False,
    )
```

```python
import functools
import math

import jax
import jax.numpy as jnp
import numpy as np
from jax import lax
from jax.experimental import pallas as pl
from jax.experimental.pallas import tpu as pltpu
from jax.sharding import PartitionSpec as P


D = 4096
EPSILON = 1e-05
OUTER = 32
INNER = 128
LENGTH = OUTER * INNER
BF16 = jnp.bfloat16
F32 = jnp.float32


def tables():
    m = np.arange(INNER, dtype=np.float64)
    turn = 2.0 * np.pi * (np.arange(OUTER)[:, None] + 0.25) * m[None, :] / LENGTH
    angle = 2.0 * np.pi * ((m[:, None] * m[None, :]) % INNER) / INNER
    cos, sin = np.cos(angle), np.sin(angle)
    ahead = np.block([[cos, -sin], [sin, cos]])
    back = np.block([[cos, sin], [-sin, cos]])
    parts = []
    for table in (ahead, back):
        upper = table.astype(BF16)
        lower = (table - upper.astype(np.float64)).astype(BF16)
        parts.append(np.concatenate([upper, lower, upper]))
    return [np.stack([np.cos(turn), -np.sin(turn)]).astype(np.float32), np.stack(parts)]


def turned(value, step, total, sign):
    re, im = value
    step %= total
    if step == 0:
        return re, im
    if 4 * step == total:
        return (-im, re) if sign > 0 else (im, -re)
    half = math.sqrt(0.5)
    if 8 * step == total:
        return ((re - im) * half, (re + im) * half) if sign > 0 else ((re + im) * half, (im - re) * half)
    if 8 * step == 3 * total:
        if sign > 0:
            return (re + im) * -half, (re - im) * half
        return (im - re) * half, (re + im) * -half
    cos = math.cos(2.0 * math.pi * step / total)
    sin = sign * math.sin(2.0 * math.pi * step / total)
    return re * cos - im * sin, re * sin + im * cos


def transform(values, sign):
    total = len(values)
    if total == 1:
        return values
    even, odd = transform(values[0::2], sign), transform(values[1::2], sign)
    first, second = [], []
    for k in range(total // 2):
        er, ei = even[k]
        dr, di = turned(odd[k], k, total, sign)
        first.append((er + dr, ei + di))
        second.append((er - dr, ei - di))
    return first + second


def in_two_passes(load, store, half_ref, sign):
    for q in range(4):
        for k, value in enumerate(transform([load(4 * p + q) for p in range(8)], sign)):
            half_ref[q, k, 0], half_ref[q, k, 1] = turned(value, q * k, OUTER, sign)
    for k in range(8):
        for j, value in enumerate(transform([(half_ref[q, k, 0], half_ref[q, k, 1]) for q in range(4)], sign)):
            store(k + 8 * j, value)


def groups_of_rows(body):
    for g in range(4):
        body(slice(8 * g, 8 * g + 8), g)


def outer_ahead(time_ref, mid_ref, half_ref, twr_ref, twi_ref):
    def group(rows, g):
        def load(n):
            x = time_ref[n, rows, :]
            angle = 2.0 * math.pi * n / (4 * OUTER)
            return x * math.cos(angle), x * -math.sin(angle)

        def store(k, value):
            re, im = value
            tr, ti = twr_ref[k : k + 1, :], twi_ref[k : k + 1, :]
            mid_ref[k, rows, 0:INNER] = re * tr - im * ti
            mid_ref[k, rows, INNER:] = re * ti + im * tr

        in_two_passes(load, store, half_ref.at[g], -1)

    groups_of_rows(group)


def outer_back(mid_ref, time_ref, half_ref, twr_ref, twi_ref):
    def group(rows, g):
        def load(k):
            re, im = mid_ref[k, rows, 0:INNER], mid_ref[k, rows, INNER:]
            tr, ti = twr_ref[k : k + 1, :], twi_ref[k : k + 1, :]
            return re * tr + im * ti, im * tr - re * ti

        def store(n, value):
            re, im = value
            angle = 2.0 * math.pi * n / (4 * OUTER)
            time_ref[n, rows, :] = re * (math.cos(angle) / LENGTH) - im * (math.sin(angle) / LENGTH)

        in_two_passes(load, store, half_ref.at[g], 1)

    groups_of_rows(group)


def product(rows, table_ref):
    upper = rows.astype(BF16)
    lower = (rows - upper.astype(F32)).astype(BF16)
    return jnp.dot(jnp.concatenate([upper, upper, lower], axis=1), table_ref[...], preferred_element_type=F32)


def complex_product(a, b):
    ar, ai, br, bi = a[:, :INNER], a[:, INNER:], b[:, :INNER], b[:, INNER:]
    return jnp.concatenate([ar * br - ai * bi, ar * bi + ai * br], axis=1)


def chunks(body):
    def step(j, carry):
        body(pl.ds(pl.multiple_of(j * 8, 8), 8))
        return carry

    lax.fori_loop(0, OUTER // 8, step, 0)


def flat(value):
    return value.reshape(value.shape[0] * value.shape[1], value.shape[2])


def column_of(row_ref, first):
    total = row_ref.shape[1]
    lane = lax.broadcasted_iota(jnp.int32, (32, total), 1)
    wanted = lax.broadcasted_iota(jnp.int32, (32, total), 0) + first
    return jnp.sum(jnp.where(lane == wanted, row_ref[...], 0.0), axis=1, keepdims=True)


def filter_kernel(
    got_ref,
    taps_ref,
    bias_ref,
    turn_hbm,
    inner_hbm,
    spec_hbm,
    time_ref,
    mid_ref,
    half_ref,
    turn_ref,
    inner_ref,
    sems,
    spec_ref,
    out_sems,
):
    turn_copy, inner_copy = fetch((turn_hbm, inner_hbm), (turn_ref, inner_ref), sems)
    twr_ref, twi_ref, ahead, back = turn_ref.at[0], turn_ref.at[1], inner_ref.at[0], inner_ref.at[1]
    first = pl.multiple_of(lax.axis_index("seq") * 32, 32)
    bias = column_of(bias_ref, first)
    own_taps = taps_ref[pl.ds(first, 32), :]
    for b in range(16):
        for h in range(2):
            time_ref[2 * b + h] = got_ref[b, 0:32, h * INNER : (h + 1) * INNER].astype(F32)
    turn_copy.wait()
    outer_ahead(time_ref, mid_ref, half_ref, twr_ref, twi_ref)
    inner_copy.wait()

    def combine(ks):
        long = product(flat(mid_ref[ks]), ahead)
        lift = jnp.concatenate([jnp.broadcast_to(bias, (32, INNER)), jnp.zeros((32, INNER), F32)], axis=1)
        long = long + jnp.tile(lift, (8, 1))
        taps = own_taps[None]
        tr, ti = twr_ref[ks, :][:, None, :], twi_ref[ks, :][:, None, :]
        short = product(flat(jnp.concatenate([taps * tr, taps * ti], axis=2)), ahead)
        mid_ref[ks] = product(complex_product(long, short), back).reshape(8, 32, 2 * INNER)

    chunks(combine)
    outer_back(mid_ref, time_ref, half_ref, twr_ref, twi_ref)
    outer_ahead(time_ref, mid_ref, half_ref, twr_ref, twi_ref)

    copies = []
    for j in range(OUTER // 8):
        ks = slice(8 * j, 8 * j + 8)
        spec_ref[ks] = product(flat(mid_ref[ks]), ahead).reshape(8, 32, 2 * INNER)
        copies.append(pltpu.make_async_copy(spec_ref.at[ks], spec_hbm.at[ks], out_sems.at[j]))
        copies[-1].start()
    for copy in copies:
        copy.wait()


def signal_kernel(
    got_ref, spec_hbm, turn_hbm, inner_hbm, mixed_ref, time_ref, mid_ref, half_ref, turn_ref, inner_ref, sems, spec_ref
):
    copies = fetch((turn_hbm, inner_hbm, spec_hbm), (turn_ref, inner_ref, spec_ref), sems)
    twr_ref, twi_ref, ahead, back = turn_ref.at[0], turn_ref.at[1], inner_ref.at[0], inner_ref.at[1]
    for b in range(16):
        for h in range(2):
            time_ref[2 * b + h] = got_ref[b, 0:32, h * INNER : (h + 1) * INNER].astype(F32)
    copies[0].wait()
    outer_ahead(time_ref, mid_ref, half_ref, twr_ref, twi_ref)
    copies[1].wait()
    copies[2].wait()

    def combine(ks):
        spec = product(flat(mid_ref[ks]), ahead)
        joint = complex_product(spec, flat(spec_ref[ks]))
        mid_ref[ks] = product(joint, back).reshape(8, 32, 2 * INNER)

    chunks(combine)
    outer_back(mid_ref, time_ref, half_ref, twr_ref, twi_ref)
    for b in range(16):
        for h in range(2):
            cols = slice(h * INNER, (h + 1) * INNER)
            long_out = time_ref[2 * b + h].astype(BF16).astype(F32)
            mixed_ref[b, :, cols] = (got_ref[b, 32:64, cols].astype(F32) * long_out).astype(BF16)


def vmem(count):
    return [pl.BlockSpec(memory_space=pltpu.VMEM)] * count


def hbm(count):
    return [pl.BlockSpec(memory_space=pltpu.HBM)] * count


def stay(value):
    return pltpu.with_memory_space_constraint(value, pltpu.HBM)


def fetch(sources, targets, sems):
    copies = [pltpu.make_async_copy(source, target, sems.at[i]) for i, (source, target) in enumerate(zip(sources, targets))]
    for copy in copies:
        copy.start()
    return copies


SCRATCH = [
    pltpu.VMEM((OUTER, 32, INNER), F32),
    pltpu.VMEM((OUTER, 32, 2 * INNER), F32),
    pltpu.VMEM((4, 4, 8, 2, 8, INNER), F32),
    pltpu.VMEM((2, OUTER, INNER), F32),
    pltpu.VMEM((2, 6 * INNER, 2 * INNER), BF16),
    pltpu.SemaphoreType.DMA((3,)),
]


def filter_spectrum(got, taps, bias, consts):
    return pl.pallas_call(
        filter_kernel,
        out_shape=pltpu.HBM((OUTER, 32, 2 * INNER), F32),
        in_specs=vmem(3) + hbm(2),
        out_specs=hbm(1)[0],
        scratch_shapes=[*SCRATCH, pltpu.VMEM((OUTER, 32, 2 * INNER), F32), pltpu.SemaphoreType.DMA((4,))],
        cost_estimate=pl.CostEstimate(flops=2_000_000_000, bytes_accessed=3_000_000, transcendentals=0),
        compiler_params=limit(8),
        name="filter_spectrum",
    )(got, taps, bias, *[stay(value) for value in consts])


def gated_convolution(got, spec, consts):
    return pl.pallas_call(
        signal_kernel,
        out_shape=jax.ShapeDtypeStruct((16, 32, 256), BF16),
        in_specs=vmem(1) + hbm(3),
        out_specs=vmem(1)[0],
        scratch_shapes=[*SCRATCH, pltpu.VMEM((OUTER, 32, 2 * INNER), F32)],
        cost_estimate=pl.CostEstimate(flops=1_000_000_000, bytes_accessed=3_000_000, transcendentals=0),
        compiler_params=limit(8),
    )(got, stay(spec), *[stay(value) for value in consts])


def pack_kernel(hidden_hbm, long_ref, up_ref, gain_hbm, payload_ref, squares_ref, lifted_ref, hidden, gain_ref, sems):
    chan = lax.axis_index("chan")
    pair = [pl.ds(pl.multiple_of((lax.bitwise_and(chan, 3) + 4 * z) * 32, 32), 32) for z in range(2)]
    sources = [gain_hbm, hidden_hbm, long_ref, up_ref.at[:, pair[0], :], up_ref.at[:, pair[1], :]]
    targets = [gain_ref, hidden, *[payload_ref.at[:, 32 * i : 32 * i + 32, :] for i in range(3)]]
    copies = fetch(sources, targets, sems)
    copies[0].wait()
    gains = [jnp.broadcast_to(gain_ref[q : q + 1, :], (INNER, INNER)).T for q in range(4)]
    copies[1].wait()
    total = jnp.zeros((8, 256), F32)
    for b in range(16):
        states = hidden[b].astype(F32)
        powers = states * states
        for r in range(4):
            total = total + powers[8 * r : 8 * r + 8]
        gain = gains[b // 4][32 * (b % 4) : 32 * (b % 4) + 32]
        lifted_ref[b] = states * jnp.concatenate([gain, gain], axis=1)
    squares_ref[...] = total
    for copy in copies[2:]:
        copy.wait()


def norm_kernel(lifted_ref, s0, s1, s2, s3, gate_hbm, payload_ref, sems):
    (copy,) = fetch([gate_hbm], [payload_ref.at[:, 32:64, :]], sems)
    squares = (s0[...] + s1[...]) + (s2[...] + s3[...])
    scale = lax.rsqrt(jnp.sum(squares, axis=0, keepdims=True) / D + EPSILON)
    for b in range(16):
        payload_ref[b, 0:32, :] = (lifted_ref[b] * scale).astype(BF16)
    copy.wait()


def limit(mib):
    return pltpu.CompilerParams(vmem_limit_bytes=mib * 2**20)


def pack(hidden, long_filter, upstream, gain):
    return pl.pallas_call(
        pack_kernel,
        out_shape=(
            jax.ShapeDtypeStruct((16, 96, 256), BF16),
            jax.ShapeDtypeStruct((8, 256), F32),
            jax.ShapeDtypeStruct((16, 32, 256), F32),
        ),
        in_specs=hbm(4),
        out_specs=tuple(vmem(3)),
        scratch_shapes=[
            pltpu.VMEM((16, 32, 256), BF16),
            pltpu.VMEM((4, INNER), F32),
            pltpu.SemaphoreType.DMA((5,)),
        ],
        compiler_params=limit(6),
        name="pack",
    )(stay(hidden), stay(long_filter), stay(upstream), stay(gain))


def normalise(lifted, squares, gate):
    return pl.pallas_call(
        norm_kernel,
        out_shape=jax.ShapeDtypeStruct((16, 64, 256), BF16),
        in_specs=vmem(5) + hbm(1),
        out_specs=vmem(1)[0],
        scratch_shapes=[pltpu.SemaphoreType.DMA((1,))],
        compiler_params=limit(6),
        name="normalise",
    )(lifted, *squares, stay(gate))


def place_of(s):
    return s // 8, (s // 2) % 4, s % 2


def over_seq(value, dz, dx, dk):
    pairs = []
    for s in range(16):
        z, x, k = place_of(s)
        pairs.append((s, (z ^ dz) * 8 + ((x + dx) % 4) * 2 + (k ^ dk)))
    return lax.ppermute(value, "seq", pairs)


def over_chan(value, dz, dy):
    pairs = [(c, ((c // 4) ^ dz) * 4 + (c + dy) % 4) for c in range(8)]
    return lax.ppermute(value, "chan", pairs)


def gather_seq(own):
    side = over_seq(own, 1, 0, 0)
    near = {(0, 0): own, (1, 0): side}
    for dx in (3, 1, 2):
        near[0, dx] = over_seq(own, 0, -dx, 0)
    for dx in (3, 1):
        near[1, dx] = over_seq(side, 0, -dx, 0)
    near[1, 2] = over_seq(near[0, 2], 1, 0, 0)
    pieces = []
    for (dz, dx), value in near.items():
        pieces += [(value, 0, dz, dx), (over_seq(value, 0, 0, 1), 1, dz, dx)]
    return pieces


def gather_chan(own):
    pieces = [(own, 0)]
    for dy in (3, 1, 2):
        pieces.append((over_chan(own, 0, -dy), dy))
    return pieces


def whole_rows(refs):
    return jnp.concatenate([jnp.concatenate([ref[b] for b in range(16)], axis=1) for ref in refs], axis=0)


def grad_kernel(mixed_keys, up_keys, *refs):
    seq, chan = lax.axis_index("seq"), lax.axis_index("chan")
    mixed_refs, up_refs = refs[: len(mixed_keys)], refs[len(mixed_keys) : len(mixed_keys) + len(up_keys)]
    mixed_ref, grad_ref, rows_ref = refs[len(mixed_keys) + len(up_keys) :]
    total = lax.dot_general(whole_rows(mixed_refs), whole_rows(up_refs), (((1,), (1,)), ((), ())), preferred_element_type=F32)

    def source_place(dk, dz, dx):
        z = lax.bitwise_xor(seq // 8, dz)
        x = lax.bitwise_and(seq // 2 + dx, 3)
        k = lax.bitwise_xor(lax.bitwise_and(seq, 1), dk)
        return pl.ds(pl.multiple_of((z * 8 + x * 2 + k) * 32, 32), 32)

    for i, (ref, key) in enumerate(zip(mixed_refs, mixed_keys, strict=True)):
        place = source_place(*key)
        rows_ref[place, :] = total[32 * i : 32 * i + 32]
        mixed_ref[place, :] = ref[seq]
    turned_rows = rows_ref[...].T
    for i, (dy,) in enumerate(up_keys):
        for z in range(2):
            place = pl.ds(pl.multiple_of((4 * z + lax.bitwise_and(chan + dy, 3)) * 32, 32), 32)
            grad_ref[place, :] = turned_rows[64 * i + 32 * z : 64 * i + 32 * z + 32]


def weight_gradient(mixed, up):
    mixed_keys, up_keys = [piece[1:] for piece in mixed], [piece[1:] for piece in up]
    return pl.pallas_call(
        functools.partial(grad_kernel, mixed_keys, up_keys),
        out_shape=(jax.ShapeDtypeStruct((512, 256), BF16), jax.ShapeDtypeStruct((256, 512), F32)),
        in_specs=vmem(len(mixed) + len(up)),
        out_specs=tuple(vmem(2)),
        scratch_shapes=[pltpu.VMEM((512, 256), F32)],
        cost_estimate=pl.CostEstimate(flops=1_000_000_000, bytes_accessed=7_000_000, transcendentals=0),
        compiler_params=limit(16),
        name="weight_gradient",
    )(*[piece[0] for piece in mixed], *[piece[0] for piece in up])


def exchange(value, axis):
    return lax.all_to_all(value, axis, split_axis=0, concat_axis=0, tiled=True)


def step(hidden_states, norm_gain, short_filter, long_filter, long_bias, gate_stream, upstream):
    consts = [jnp.asarray(table) for table in tables()]
    hidden, filt, gate = [value.reshape(16, 32, 256) for value in (hidden_states, long_filter, gate_stream)]
    payload, squares, lifted = pack(hidden, filt, upstream.reshape(16, 256, 256), norm_gain.reshape(4, INNER))
    squares = squares + over_chan(squares, 1, 0)
    got = exchange(payload, "seq")
    parts = [squares]
    for dy in (1, 3, 2):
        parts.append(over_chan(squares, 0, dy))
    payload = normalise(lifted, parts, gate)
    signal = exchange(payload, "seq")
    spec = filter_spectrum(got, short_filter, long_bias[None, :], consts)
    up = gather_chan(got[:, 32:96])
    mixed = gated_convolution(signal, spec, consts)
    return weight_gradient(gather_seq(mixed), up)


def solution(mesh):
    placed = (
        P("chan", "seq"),
        P("chan"),
        P("chan", None),
        P("chan", "seq"),
        P("chan"),
        P("chan", "seq"),
        P(None, "seq"),
    )
    return jax.shard_map(
        step,
        mesh=mesh,
        in_specs=placed,
        out_specs=(P("chan", "seq"), P("seq", "chan")),
        check_vma=False,
    )
```

```python
import functools
import math

import jax
import jax.numpy as jnp
import numpy as np
from jax import lax
from jax.experimental import pallas as pl
from jax.experimental.pallas import tpu as pltpu
from jax.sharding import PartitionSpec as P


D = 4096
EPSILON = 1e-05
OUTER = 32
INNER = 128
LENGTH = OUTER * INNER
BF16 = jnp.bfloat16
F32 = jnp.float32


def tables():
    m = np.arange(INNER, dtype=np.float64)
    turn = 2.0 * np.pi * (np.arange(OUTER)[:, None] + 0.25) * m[None, :] / LENGTH
    angle = 2.0 * np.pi * ((m[:, None] * m[None, :]) % INNER) / INNER
    cos, sin = np.cos(angle), np.sin(angle)
    ahead = np.block([[cos, -sin], [sin, cos]])
    back = np.block([[cos, sin], [-sin, cos]])
    parts = []
    for table in (ahead, back):
        upper = table.astype(BF16)
        lower = (table - upper.astype(np.float64)).astype(BF16)
        parts.append(np.concatenate([upper, lower]))
    return [np.stack([np.cos(turn), -np.sin(turn)]).astype(np.float32), np.stack(parts)]


def turned(value, step, total, sign):
    re, im = value
    step %= total
    if step == 0:
        return re, im
    if 4 * step == total:
        return (-im, re) if sign > 0 else (im, -re)
    half = math.sqrt(0.5)
    if 8 * step == total:
        return ((re - im) * half, (re + im) * half) if sign > 0 else ((re + im) * half, (im - re) * half)
    if 8 * step == 3 * total:
        if sign > 0:
            return (re + im) * -half, (re - im) * half
        return (im - re) * half, (re + im) * -half
    cos = math.cos(2.0 * math.pi * step / total)
    sin = sign * math.sin(2.0 * math.pi * step / total)
    return re * cos - im * sin, re * sin + im * cos


def transform(values, sign):
    total = len(values)
    if total == 1:
        return values
    even, odd = transform(values[0::2], sign), transform(values[1::2], sign)
    first, second = [], []
    for k in range(total // 2):
        er, ei = even[k]
        dr, di = turned(odd[k], k, total, sign)
        first.append((er + dr, ei + di))
        second.append((er - dr, ei - di))
    return first + second


def first_pass(load, half_ref, sign):
    for q in range(4):
        for k, value in enumerate(transform([load(4 * p + q) for p in range(8)], sign)):
            half_ref[q, k, 0], half_ref[q, k, 1] = turned(value, q * k, OUTER, sign)


def second_pass(store, half_ref, sign):
    for k in range(8):
        for j, value in enumerate(transform([(half_ref[q, k, 0], half_ref[q, k, 1]) for q in range(4)], sign)):
            store(k + 8 * j, value)


def row_groups():
    return [(g, slice(8 * g, 8 * g + 8)) for g in range(4)]


def outer_ahead(time_ref, mid_ref, half_ref, turn_ref, ready=None):
    for g, rows in row_groups():

        def load(n, rows=rows):
            x = time_ref[n, rows, :]
            angle = 2.0 * math.pi * n / (4 * OUTER)
            return x * math.cos(angle), x * -math.sin(angle)

        first_pass(load, half_ref.at[g], -1)
    if ready is not None:
        ready.wait()
    for g, rows in row_groups():

        def store(k, value, rows=rows):
            re, im = value
            tr, ti = turn_ref[0, k : k + 1, :], turn_ref[1, k : k + 1, :]
            mid_ref[k, rows, 0:INNER] = re * tr - im * ti
            mid_ref[k, rows, INNER:] = re * ti + im * tr

        second_pass(store, half_ref.at[g], -1)


def outer_back(mid_ref, time_ref, half_ref, turn_ref):
    for g, rows in row_groups():

        def load(k, rows=rows):
            re, im = mid_ref[k, rows, 0:INNER], mid_ref[k, rows, INNER:]
            tr, ti = turn_ref[0, k : k + 1, :], turn_ref[1, k : k + 1, :]
            return re * tr + im * ti, im * tr - re * ti

        def store(n, value, rows=rows):
            re, im = value
            angle = 2.0 * math.pi * n / (4 * OUTER)
            time_ref[n, rows, :] = re * (math.cos(angle) / LENGTH) - im * (math.sin(angle) / LENGTH)

        first_pass(load, half_ref.at[g], 1)
        second_pass(store, half_ref.at[g], 1)


def product(rows, table_ref):
    upper = rows.astype(BF16)
    lower = (rows - upper.astype(F32)).astype(BF16)
    dot = functools.partial(jnp.dot, preferred_element_type=F32)
    return dot(jnp.concatenate([upper, upper], axis=1), table_ref[...]) + dot(lower, table_ref[0 : 2 * INNER])


def complex_product(a, b):
    ar, ai, br, bi = a[:, :INNER], a[:, INNER:], b[:, :INNER], b[:, INNER:]
    return jnp.concatenate([ar * br - ai * bi, ar * bi + ai * br], axis=1)


CHUNK = 16


def chunks():
    return [slice(k, k + CHUNK) for k in range(0, OUTER, CHUNK)]


def flat(value):
    return value.reshape(value.shape[0] * value.shape[1], value.shape[2])


def column_of(row_ref, first):
    total = row_ref.shape[1]
    lane = lax.broadcasted_iota(jnp.int32, (32, total), 1)
    wanted = lax.broadcasted_iota(jnp.int32, (32, total), 0) + first
    return jnp.sum(jnp.where(lane == wanted, row_ref[...], 0.0), axis=1, keepdims=True)


def filter_kernel(
    got_ref,
    taps_hbm,
    bias_ref,
    turn_hbm,
    inner_hbm,
    spec_hbm,
    time_ref,
    mid_ref,
    half_ref,
    turn_ref,
    inner_ref,
    spec_ref,
    sems,
    spec_sems,
    taps_ref,
):
    first = pl.multiple_of(lax.axis_index("seq") * 32, 32)
    sources = (turn_hbm, taps_hbm.at[pl.ds(first, 32), :], inner_hbm)
    copies = fetch(sources, (turn_ref, taps_ref, inner_ref), sems)
    ahead, back = inner_ref.at[0], inner_ref.at[1]
    for b in range(16):
        for h in range(2):
            time_ref[2 * b + h] = got_ref[b, 0:32, h * INNER : (h + 1) * INNER].astype(F32)
    bias = column_of(bias_ref, first)
    lift = jnp.concatenate([jnp.broadcast_to(bias, (32, INNER)), jnp.zeros((32, INNER), F32)], axis=1)
    outer_ahead(time_ref, mid_ref, half_ref, turn_ref, copies[0])
    copies[1].wait()
    copies[2].wait()
    for ks in chunks():
        long = product(flat(mid_ref[ks]), ahead)
        long = long + jnp.tile(lift, (CHUNK, 1))
        taps = taps_ref[...][None]
        tr, ti = turn_ref[0, ks, :][:, None, :], turn_ref[1, ks, :][:, None, :]
        short = product(flat(jnp.concatenate([taps * tr, taps * ti], axis=2)), ahead)
        mid_ref[ks] = product(complex_product(long, short), back).reshape(CHUNK, 32, 2 * INNER)
    outer_back(mid_ref, time_ref, half_ref, turn_ref)
    outer_ahead(time_ref, mid_ref, half_ref, turn_ref)
    written = []
    for j, ks in enumerate(chunks()):
        spec_ref[ks] = product(flat(mid_ref[ks]), ahead).reshape(CHUNK, 32, 2 * INNER)
        written.append(pltpu.make_async_copy(spec_ref.at[ks], spec_hbm.at[ks], spec_sems.at[j]))
        written[-1].start()
    for copy in written:
        copy.wait()


def signal_kernel(
    got_ref,
    spec_hbm,
    turn_hbm,
    inner_hbm,
    mixed_ref,
    time_ref,
    mid_ref,
    half_ref,
    turn_ref,
    inner_ref,
    spec_ref,
    sems,
    spec_sems,
):
    copies = fetch((turn_hbm, inner_hbm), (turn_ref, inner_ref), sems)
    spec_copies = fetch([spec_hbm.at[ks] for ks in chunks()], [spec_ref.at[ks] for ks in chunks()], spec_sems)
    ahead, back = inner_ref.at[0], inner_ref.at[1]
    for b in range(16):
        for h in range(2):
            time_ref[2 * b + h] = got_ref[b, 0:32, h * INNER : (h + 1) * INNER].astype(F32)
    outer_ahead(time_ref, mid_ref, half_ref, turn_ref, copies[0])
    copies[1].wait()
    for ks, copy in zip(chunks(), spec_copies, strict=True):
        spec = product(flat(mid_ref[ks]), ahead)
        copy.wait()
        joint = complex_product(spec, flat(spec_ref[ks]))
        mid_ref[ks] = product(joint, back).reshape(CHUNK, 32, 2 * INNER)
    outer_back(mid_ref, time_ref, half_ref, turn_ref)
    for b in range(16):
        for h in range(2):
            cols = slice(h * INNER, (h + 1) * INNER)
            long_out = time_ref[2 * b + h].astype(BF16).astype(F32)
            mixed_ref[b, :, cols] = (got_ref[b, 32:64, cols].astype(F32) * long_out).astype(BF16)


def vmem(count):
    return [pl.BlockSpec(memory_space=pltpu.VMEM)] * count


def hbm(count):
    return [pl.BlockSpec(memory_space=pltpu.HBM)] * count


def stay(value):
    return pltpu.with_memory_space_constraint(value, pltpu.HBM)


def fetch(sources, targets, sems):
    copies = [pltpu.make_async_copy(source, target, sems.at[i]) for i, (source, target) in enumerate(zip(sources, targets))]
    for copy in copies:
        copy.start()
    return copies


SCRATCH = [
    pltpu.VMEM((OUTER, 32, INNER), F32),
    pltpu.VMEM((OUTER, 32, 2 * INNER), F32),
    pltpu.VMEM((4, 4, 8, 2, 8, INNER), F32),
    pltpu.VMEM((2, OUTER, INNER), F32),
    pltpu.VMEM((2, 4 * INNER, 2 * INNER), BF16),
    pltpu.VMEM((OUTER, 32, 2 * INNER), F32),
    pltpu.SemaphoreType.DMA((3,)),
    pltpu.SemaphoreType.DMA((OUTER // CHUNK,)),
]


def filter_spectrum(got, taps, bias, consts):
    return pl.pallas_call(
        filter_kernel,
        out_shape=pltpu.HBM((OUTER, 32, 2 * INNER), F32),
        in_specs=[*vmem(1), *hbm(1), *vmem(1), *hbm(2)],
        out_specs=hbm(1)[0],
        scratch_shapes=[*SCRATCH, pltpu.VMEM((32, INNER), F32)],
        cost_estimate=pl.CostEstimate(flops=2_000_000_000, bytes_accessed=3_000_000, transcendentals=0),
        compiler_params=limit(8),
        name="filter_spectrum",
    )(got, stay(taps), bias, *[stay(value) for value in consts])


def gated_convolution(got, spec, consts):
    return pl.pallas_call(
        signal_kernel,
        out_shape=jax.ShapeDtypeStruct((16, 32, 256), BF16),
        in_specs=vmem(1) + hbm(3),
        out_specs=vmem(1)[0],
        scratch_shapes=SCRATCH,
        cost_estimate=pl.CostEstimate(flops=1_000_000_000, bytes_accessed=3_000_000, transcendentals=0),
        compiler_params=limit(8),
    )(got, stay(spec), *[stay(value) for value in consts])


def pack_kernel(hidden_hbm, long_ref, up_ref, gain_hbm, payload_ref, squares_ref, lifted_ref, hidden, gain_ref, sems):
    chan = lax.axis_index("chan")
    pair = [pl.ds(pl.multiple_of((lax.bitwise_and(chan, 3) + 4 * z) * 32, 32), 32) for z in range(2)]
    sources = [gain_hbm, hidden_hbm, long_ref, up_ref.at[:, pair[0], :], up_ref.at[:, pair[1], :]]
    targets = [gain_ref, hidden, *[payload_ref.at[:, 32 * i : 32 * i + 32, :] for i in range(3)]]
    copies = fetch(sources, targets, sems)
    copies[0].wait()
    gains = [jnp.broadcast_to(gain_ref[q : q + 1, :], (INNER, INNER)).T for q in range(4)]
    copies[1].wait()
    total = jnp.zeros((8, 256), F32)
    for b in range(16):
        states = hidden[b].astype(F32)
        powers = states * states
        for r in range(4):
            total = total + powers[8 * r : 8 * r + 8]
        gain = gains[b // 4][32 * (b % 4) : 32 * (b % 4) + 32]
        lifted_ref[b] = states * jnp.concatenate([gain, gain], axis=1)
    squares_ref[...] = total
    for copy in copies[2:]:
        copy.wait()


def norm_kernel(lifted_ref, s0, s1, s2, s3, gate_hbm, payload_ref, sems):
    (copy,) = fetch([gate_hbm], [payload_ref.at[:, 32:64, :]], sems)
    squares = (s0[...] + s1[...]) + (s2[...] + s3[...])
    scale = lax.rsqrt(jnp.sum(squares, axis=0, keepdims=True) / D + EPSILON)
    for b in range(16):
        payload_ref[b, 0:32, :] = (lifted_ref[b] * scale).astype(BF16)
    copy.wait()


def limit(mib):
    return pltpu.CompilerParams(vmem_limit_bytes=mib * 2**20)


def pack(hidden, long_filter, upstream, gain):
    return pl.pallas_call(
        pack_kernel,
        out_shape=(
            jax.ShapeDtypeStruct((16, 96, 256), BF16),
            jax.ShapeDtypeStruct((8, 256), F32),
            jax.ShapeDtypeStruct((16, 32, 256), F32),
        ),
        in_specs=hbm(4),
        out_specs=tuple(vmem(3)),
        scratch_shapes=[
            pltpu.VMEM((16, 32, 256), BF16),
            pltpu.VMEM((4, INNER), F32),
            pltpu.SemaphoreType.DMA((5,)),
        ],
        compiler_params=limit(6),
        name="pack",
    )(stay(hidden), stay(long_filter), stay(upstream), stay(gain))


def normalise(lifted, squares, gate):
    return pl.pallas_call(
        norm_kernel,
        out_shape=jax.ShapeDtypeStruct((16, 64, 256), BF16),
        in_specs=vmem(5) + hbm(1),
        out_specs=vmem(1)[0],
        scratch_shapes=[pltpu.SemaphoreType.DMA((1,))],
        compiler_params=limit(6),
        name="normalise",
    )(lifted, *squares, stay(gate))


def place_of(s):
    return s // 8, (s // 2) % 4, s % 2


def over_seq(value, dz, dx, dk):
    pairs = []
    for s in range(16):
        z, x, k = place_of(s)
        pairs.append((s, (z ^ dz) * 8 + ((x + dx) % 4) * 2 + (k ^ dk)))
    return lax.ppermute(value, "seq", pairs)


def over_chan(value, dz, dy):
    pairs = [(c, ((c // 4) ^ dz) * 4 + (c + dy) % 4) for c in range(8)]
    return lax.ppermute(value, "chan", pairs)


def gather_seq(own):
    side = over_seq(own, 1, 0, 0)
    near = {(0, 0): own, (1, 0): side}
    for dx in (3, 1, 2):
        near[0, dx] = over_seq(own, 0, -dx, 0)
    for dx in (3, 1):
        near[1, dx] = over_seq(side, 0, -dx, 0)
    near[1, 2] = over_seq(near[0, 2], 1, 0, 0)
    pieces = []
    for (dz, dx), value in near.items():
        pieces += [(value, 0, dz, dx), (over_seq(value, 0, 0, 1), 1, dz, dx)]
    return pieces


def gather_chan(own):
    pieces = [(own, 0)]
    for dy in (3, 1, 2):
        pieces.append((over_chan(own, 0, -dy), dy))
    return pieces


def whole_rows(refs):
    return jnp.concatenate([jnp.concatenate([ref[b] for b in range(16)], axis=1) for ref in refs], axis=0)


def grad_kernel(mixed_keys, up_keys, *refs):
    seq, chan = lax.axis_index("seq"), lax.axis_index("chan")
    mixed_refs, up_refs = refs[: len(mixed_keys)], refs[len(mixed_keys) : len(mixed_keys) + len(up_keys)]
    mixed_ref, grad_ref, rows_ref = refs[len(mixed_keys) + len(up_keys) :]
    total = lax.dot_general(whole_rows(mixed_refs), whole_rows(up_refs), (((1,), (1,)), ((), ())), preferred_element_type=F32)

    def source_place(dk, dz, dx):
        z = lax.bitwise_xor(seq // 8, dz)
        x = lax.bitwise_and(seq // 2 + dx, 3)
        k = lax.bitwise_xor(lax.bitwise_and(seq, 1), dk)
        return pl.ds(pl.multiple_of((z * 8 + x * 2 + k) * 32, 32), 32)

    for i, (ref, key) in enumerate(zip(mixed_refs, mixed_keys, strict=True)):
        place = source_place(*key)
        rows_ref[place, :] = total[32 * i : 32 * i + 32]
        mixed_ref[place, :] = ref[seq]
    turned_rows = rows_ref[...].T
    for i, (dy,) in enumerate(up_keys):
        for z in range(2):
            place = pl.ds(pl.multiple_of((4 * z + lax.bitwise_and(chan + dy, 3)) * 32, 32), 32)
            grad_ref[place, :] = turned_rows[64 * i + 32 * z : 64 * i + 32 * z + 32]


def weight_gradient(mixed, up):
    mixed_keys, up_keys = [piece[1:] for piece in mixed], [piece[1:] for piece in up]
    return pl.pallas_call(
        functools.partial(grad_kernel, mixed_keys, up_keys),
        out_shape=(jax.ShapeDtypeStruct((512, 256), BF16), jax.ShapeDtypeStruct((256, 512), F32)),
        in_specs=vmem(len(mixed) + len(up)),
        out_specs=tuple(vmem(2)),
        scratch_shapes=[pltpu.VMEM((512, 256), F32)],
        cost_estimate=pl.CostEstimate(flops=1_000_000_000, bytes_accessed=7_000_000, transcendentals=0),
        compiler_params=limit(16),
        name="weight_gradient",
    )(*[piece[0] for piece in mixed], *[piece[0] for piece in up])


def exchange(value, axis):
    return lax.all_to_all(value, axis, split_axis=0, concat_axis=0, tiled=True)


def step(hidden_states, norm_gain, short_filter, long_filter, long_bias, gate_stream, upstream):
    consts = [jnp.asarray(table) for table in tables()]
    hidden, filt, gate = [value.reshape(16, 32, 256) for value in (hidden_states, long_filter, gate_stream)]
    payload, squares, lifted = pack(hidden, filt, upstream.reshape(16, 256, 256), norm_gain.reshape(4, INNER))
    squares = squares + over_chan(squares, 1, 0)
    got = exchange(payload, "seq")
    parts = [squares]
    for dy in (1, 3, 2):
        parts.append(over_chan(squares, 0, dy))
    payload = normalise(lifted, parts, gate)
    signal = exchange(payload, "seq")
    spec = filter_spectrum(got, short_filter, long_bias[None, :], consts)
    up = gather_chan(got[:, 32:96])
    mixed = gated_convolution(signal, spec, consts)
    return weight_gradient(gather_seq(mixed), up)


def solution(mesh):
    placed = (
        P("chan", "seq"),
        P("chan"),
        P("chan", None),
        P("chan", "seq"),
        P("chan"),
        P("chan", "seq"),
        P(None, "seq"),
    )
    return jax.shard_map(
        step,
        mesh=mesh,
        in_specs=placed,
        out_specs=(P("chan", "seq"), P("seq", "chan")),
        check_vma=False,
    )
```

```python
import functools
import math

import jax
import jax.numpy as jnp
import numpy as np
from jax import lax
from jax.experimental import pallas as pl
from jax.experimental.pallas import tpu as pltpu
from jax.sharding import PartitionSpec as P


D = 4096
EPSILON = 1e-05
OUTER = 32
INNER = 128
LENGTH = OUTER * INNER
BF16 = jnp.bfloat16
F32 = jnp.float32


def tables():
    m = np.arange(INNER, dtype=np.float64)
    turn = 2.0 * np.pi * (np.arange(OUTER)[:, None] + 0.25) * m[None, :] / LENGTH
    angle = 2.0 * np.pi * ((m[:, None] * m[None, :]) % INNER) / INNER
    cos, sin = np.cos(angle), np.sin(angle)
    ahead = np.block([[cos, -sin], [sin, cos]])
    back = np.block([[cos, sin], [-sin, cos]])
    parts = []
    for table in (ahead, back):
        upper = table.astype(BF16)
        lower = (table - upper.astype(np.float64)).astype(BF16)
        parts.append(np.concatenate([upper, lower]))
    return [np.stack([np.cos(turn), -np.sin(turn)]).astype(np.float32), np.stack(parts)]


def turned(value, step, total, sign):
    re, im = value
    step %= total
    if step == 0:
        return re, im
    if 4 * step == total:
        return (-im, re) if sign > 0 else (im, -re)
    half = math.sqrt(0.5)
    if 8 * step == total:
        return ((re - im) * half, (re + im) * half) if sign > 0 else ((re + im) * half, (im - re) * half)
    if 8 * step == 3 * total:
        if sign > 0:
            return (re + im) * -half, (re - im) * half
        return (im - re) * half, (re + im) * -half
    cos = math.cos(2.0 * math.pi * step / total)
    sin = sign * math.sin(2.0 * math.pi * step / total)
    return re * cos - im * sin, re * sin + im * cos


def transform(values, sign):
    total = len(values)
    if total == 1:
        return values
    even, odd = transform(values[0::2], sign), transform(values[1::2], sign)
    first, second = [], []
    for k in range(total // 2):
        er, ei = even[k]
        dr, di = turned(odd[k], k, total, sign)
        first.append((er + dr, ei + di))
        second.append((er - dr, ei - di))
    return first + second


def first_pass(load, half_ref, sign):
    for q in range(4):
        for k, value in enumerate(transform([load(4 * p + q) for p in range(8)], sign)):
            half_ref[q, k, 0], half_ref[q, k, 1] = turned(value, q * k, OUTER, sign)


def second_pass(store, half_ref, sign):
    for k in range(8):
        for j, value in enumerate(transform([(half_ref[q, k, 0], half_ref[q, k, 1]) for q in range(4)], sign)):
            store(k + 8 * j, value)


def row_groups():
    return [(g, slice(8 * g, 8 * g + 8)) for g in range(4)]


def outer_ahead(time_ref, mid_ref, half_ref, turn_ref, ready=None):
    for g, rows in row_groups():

        def load(n, rows=rows):
            x = time_ref[n, rows, :]
            angle = 2.0 * math.pi * n / (4 * OUTER)
            return x * math.cos(angle), x * -math.sin(angle)

        first_pass(load, half_ref.at[g], -1)
    if ready is not None:
        ready.wait()
    for g, rows in row_groups():

        def store(k, value, rows=rows):
            re, im = value
            tr, ti = turn_ref[0, k : k + 1, :], turn_ref[1, k : k + 1, :]
            mid_ref[k, rows, 0:INNER] = re * tr - im * ti
            mid_ref[k, rows, INNER:] = re * ti + im * tr

        second_pass(store, half_ref.at[g], -1)


def outer_back(mid_ref, time_ref, half_ref, turn_ref):
    for g, rows in row_groups():

        def load(k, rows=rows):
            re, im = mid_ref[k, rows, 0:INNER], mid_ref[k, rows, INNER:]
            tr, ti = turn_ref[0, k : k + 1, :], turn_ref[1, k : k + 1, :]
            return re * tr + im * ti, im * tr - re * ti

        def store(n, value, rows=rows):
            re, im = value
            angle = 2.0 * math.pi * n / (4 * OUTER)
            time_ref[n, rows, :] = re * (math.cos(angle) / LENGTH) - im * (math.sin(angle) / LENGTH)

        first_pass(load, half_ref.at[g], 1)
        second_pass(store, half_ref.at[g], 1)


def product(rows, table_ref):
    upper = rows.astype(BF16)
    lower = (rows - upper.astype(F32)).astype(BF16)
    dot = functools.partial(jnp.dot, preferred_element_type=F32)
    return dot(jnp.concatenate([upper, upper], axis=1), table_ref[...]) + dot(lower, table_ref[0 : 2 * INNER])


def complex_product(a, b):
    ar, ai, br, bi = a[:, :INNER], a[:, INNER:], b[:, :INNER], b[:, INNER:]
    return jnp.concatenate([ar * br - ai * bi, ar * bi + ai * br], axis=1)


CHUNK = 16


def chunks():
    return [slice(k, k + CHUNK) for k in range(0, OUTER, CHUNK)]


def flat(value):
    return value.reshape(value.shape[0] * value.shape[1], value.shape[2])


def column_of(row_ref, first):
    total = row_ref.shape[1]
    lane = lax.broadcasted_iota(jnp.int32, (32, total), 1)
    wanted = lax.broadcasted_iota(jnp.int32, (32, total), 0) + first
    return jnp.sum(jnp.where(lane == wanted, row_ref[...], 0.0), axis=1, keepdims=True)


def filter_kernel(
    got_ref,
    taps_hbm,
    bias_ref,
    turn_hbm,
    inner_hbm,
    spec_hbm,
    time_ref,
    mid_ref,
    half_ref,
    turn_ref,
    inner_ref,
    spec_ref,
    sems,
    spec_sems,
    taps_ref,
):
    first = pl.multiple_of(lax.axis_index("seq") * 32, 32)
    sources = (turn_hbm, taps_hbm.at[pl.ds(first, 32), :], inner_hbm)
    copies = fetch(sources, (turn_ref, taps_ref, inner_ref), sems)
    ahead, back = inner_ref.at[0], inner_ref.at[1]
    for b in range(16):
        for h in range(2):
            time_ref[2 * b + h] = got_ref[b, 0:32, h * INNER : (h + 1) * INNER].astype(F32)
    bias = column_of(bias_ref, first)
    lift = jnp.concatenate([jnp.broadcast_to(bias, (32, INNER)), jnp.zeros((32, INNER), F32)], axis=1)
    outer_ahead(time_ref, mid_ref, half_ref, turn_ref, copies[0])
    copies[1].wait()
    copies[2].wait()
    for ks in chunks():
        long = product(flat(mid_ref[ks]), ahead)
        long = long + jnp.tile(lift, (CHUNK, 1))
        taps = taps_ref[...][None]
        tr, ti = turn_ref[0, ks, :][:, None, :], turn_ref[1, ks, :][:, None, :]
        short = product(flat(jnp.concatenate([taps * tr, taps * ti], axis=2)), ahead)
        mid_ref[ks] = product(complex_product(long, short), back).reshape(CHUNK, 32, 2 * INNER)
    outer_back(mid_ref, time_ref, half_ref, turn_ref)
    outer_ahead(time_ref, mid_ref, half_ref, turn_ref)
    written = []
    for j, ks in enumerate(chunks()):
        spec_ref[ks] = product(flat(mid_ref[ks]), ahead).reshape(CHUNK, 32, 2 * INNER)
        written.append(pltpu.make_async_copy(spec_ref.at[ks], spec_hbm.at[ks], spec_sems.at[j]))
        written[-1].start()
    for copy in written:
        copy.wait()


def signal_kernel(
    got_ref,
    spec_hbm,
    turn_hbm,
    inner_hbm,
    mixed_ref,
    time_ref,
    mid_ref,
    half_ref,
    turn_ref,
    inner_ref,
    spec_ref,
    sems,
    spec_sems,
):
    copies = fetch((turn_hbm, inner_hbm), (turn_ref, inner_ref), sems)
    spec_copies = fetch([spec_hbm.at[ks] for ks in chunks()], [spec_ref.at[ks] for ks in chunks()], spec_sems)
    ahead, back = inner_ref.at[0], inner_ref.at[1]
    for b in range(16):
        for h in range(2):
            time_ref[2 * b + h] = got_ref[b, 0:32, h * INNER : (h + 1) * INNER].astype(F32)
    outer_ahead(time_ref, mid_ref, half_ref, turn_ref, copies[0])
    copies[1].wait()
    for ks, copy in zip(chunks(), spec_copies, strict=True):
        spec = product(flat(mid_ref[ks]), ahead)
        copy.wait()
        joint = complex_product(spec, flat(spec_ref[ks]))
        mid_ref[ks] = product(joint, back).reshape(CHUNK, 32, 2 * INNER)
    outer_back(mid_ref, time_ref, half_ref, turn_ref)
    for b in range(16):
        for h in range(2):
            cols = slice(h * INNER, (h + 1) * INNER)
            long_out = time_ref[2 * b + h].astype(BF16).astype(F32)
            mixed_ref[b, :, cols] = (got_ref[b, 32:64, cols].astype(F32) * long_out).astype(BF16)


def vmem(count):
    return [pl.BlockSpec(memory_space=pltpu.VMEM)] * count


def hbm(count):
    return [pl.BlockSpec(memory_space=pltpu.HBM)] * count


def stay(value):
    return pltpu.with_memory_space_constraint(value, pltpu.HBM)


def fetch(sources, targets, sems):
    copies = [pltpu.make_async_copy(source, target, sems.at[i]) for i, (source, target) in enumerate(zip(sources, targets))]
    for copy in copies:
        copy.start()
    return copies


SCRATCH = [
    pltpu.VMEM((OUTER, 32, INNER), F32),
    pltpu.VMEM((OUTER, 32, 2 * INNER), F32),
    pltpu.VMEM((4, 4, 8, 2, 8, INNER), F32),
    pltpu.VMEM((2, OUTER, INNER), F32),
    pltpu.VMEM((2, 4 * INNER, 2 * INNER), BF16),
    pltpu.VMEM((OUTER, 32, 2 * INNER), F32),
    pltpu.SemaphoreType.DMA((3,)),
    pltpu.SemaphoreType.DMA((OUTER // CHUNK,)),
]


def filter_spectrum(got, taps, bias, consts):
    return pl.pallas_call(
        filter_kernel,
        out_shape=pltpu.HBM((OUTER, 32, 2 * INNER), F32),
        in_specs=[*vmem(1), *hbm(1), *vmem(1), *hbm(2)],
        out_specs=hbm(1)[0],
        scratch_shapes=[*SCRATCH, pltpu.VMEM((32, INNER), F32)],
        cost_estimate=pl.CostEstimate(flops=2_000_000_000, bytes_accessed=3_000_000, transcendentals=0),
        compiler_params=limit(8),
        name="filter_spectrum",
    )(got, stay(taps), bias, *[stay(value) for value in consts])


def gated_convolution(got, spec, consts):
    return pl.pallas_call(
        signal_kernel,
        out_shape=jax.ShapeDtypeStruct((16, 32, 256), BF16),
        in_specs=vmem(1) + hbm(3),
        out_specs=vmem(1)[0],
        scratch_shapes=SCRATCH,
        cost_estimate=pl.CostEstimate(flops=1_000_000_000, bytes_accessed=3_000_000, transcendentals=0),
        compiler_params=limit(8),
    )(got, stay(spec), *[stay(value) for value in consts])


def pack_kernel(
    hidden_hbm, long_ref, up_ref, gain_hbm, payload_hbm, squares_ref, lifted_ref, hidden, gain_ref, held, sems, out_sems
):
    chan = lax.axis_index("chan")
    pair = [pl.ds(pl.multiple_of((lax.bitwise_and(chan, 3) + 4 * z) * 32, 32), 32) for z in range(2)]
    sources = [gain_hbm, hidden_hbm, long_ref, up_ref.at[:, pair[0], :], up_ref.at[:, pair[1], :]]
    targets = [gain_ref, hidden, *[held.at[i] for i in range(3)]]
    copies = fetch(sources, targets, sems)
    copies[0].wait()
    gains = [jnp.broadcast_to(gain_ref[q : q + 1, :], (INNER, INNER)).T for q in range(4)]
    leaving = []
    for i in range(3):
        copies[2 + i].wait()
        leaving.append(
            pltpu.make_async_copy(held.at[i], payload_hbm.at[:, 32 * i : 32 * i + 32, :], out_sems.at[i])
        )
        leaving[-1].start()
    copies[1].wait()
    total = jnp.zeros((8, 256), F32)
    for b in range(16):
        states = hidden[b].astype(F32)
        powers = states * states
        for r in range(4):
            total = total + powers[8 * r : 8 * r + 8]
        gain = gains[b // 4][32 * (b % 4) : 32 * (b % 4) + 32]
        lifted_ref[b] = states * jnp.concatenate([gain, gain], axis=1)
    squares_ref[...] = total
    for copy in leaving:
        copy.wait()


def norm_kernel(lifted_ref, s0, s1, s2, s3, gate_hbm, payload_ref, sems):
    (copy,) = fetch([gate_hbm], [payload_ref.at[:, 32:64, :]], sems)
    squares = (s0[...] + s1[...]) + (s2[...] + s3[...])
    scale = lax.rsqrt(jnp.sum(squares, axis=0, keepdims=True) / D + EPSILON)
    for b in range(16):
        payload_ref[b, 0:32, :] = (lifted_ref[b] * scale).astype(BF16)
    copy.wait()


def limit(mib):
    return pltpu.CompilerParams(vmem_limit_bytes=mib * 2**20)


def pack(hidden, long_filter, upstream, gain):
    return pl.pallas_call(
        pack_kernel,
        out_shape=(
            jax.ShapeDtypeStruct((16, 96, 256), BF16),
            jax.ShapeDtypeStruct((8, 256), F32),
            jax.ShapeDtypeStruct((16, 32, 256), F32),
        ),
        in_specs=hbm(4),
        out_specs=(*hbm(1), *vmem(2)),
        scratch_shapes=[
            pltpu.VMEM((16, 32, 256), BF16),
            pltpu.VMEM((4, INNER), F32),
            pltpu.VMEM((3, 16, 32, 256), BF16),
            pltpu.SemaphoreType.DMA((5,)),
            pltpu.SemaphoreType.DMA((3,)),
        ],
        compiler_params=limit(6),
        name="pack",
    )(stay(hidden), stay(long_filter), stay(upstream), stay(gain))


def normalise(lifted, squares, gate):
    return pl.pallas_call(
        norm_kernel,
        out_shape=jax.ShapeDtypeStruct((16, 64, 256), BF16),
        in_specs=vmem(5) + hbm(1),
        out_specs=vmem(1)[0],
        scratch_shapes=[pltpu.SemaphoreType.DMA((1,))],
        compiler_params=limit(6),
        name="normalise",
    )(lifted, *squares, stay(gate))


def place_of(s):
    return s // 8, (s // 2) % 4, s % 2


def over_seq(value, dz, dx, dk):
    pairs = []
    for s in range(16):
        z, x, k = place_of(s)
        pairs.append((s, (z ^ dz) * 8 + ((x + dx) % 4) * 2 + (k ^ dk)))
    return lax.ppermute(value, "seq", pairs)


def over_chan(value, dz, dy):
    pairs = [(c, ((c // 4) ^ dz) * 4 + (c + dy) % 4) for c in range(8)]
    return lax.ppermute(value, "chan", pairs)


def gather_seq(own):
    side = over_seq(own, 1, 0, 0)
    near = {(0, 0): own, (1, 0): side}
    for dx in (3, 1, 2):
        near[0, dx] = over_seq(own, 0, -dx, 0)
    for dx in (3, 1):
        near[1, dx] = over_seq(side, 0, -dx, 0)
    near[1, 2] = over_seq(near[0, 2], 1, 0, 0)
    pieces = []
    for (dz, dx), value in near.items():
        pieces += [(value, 0, dz, dx), (over_seq(value, 0, 0, 1), 1, dz, dx)]
    return pieces


def gather_chan(own):
    pieces = [(own, 0)]
    for dy in (3, 1, 2):
        pieces.append((over_chan(own, 0, -dy), dy))
    return pieces


def whole_rows(refs):
    return jnp.concatenate([jnp.concatenate([ref[b] for b in range(16)], axis=1) for ref in refs], axis=0)


def grad_kernel(mixed_keys, up_keys, *refs):
    seq, chan = lax.axis_index("seq"), lax.axis_index("chan")
    mixed_refs, up_refs = refs[: len(mixed_keys)], refs[len(mixed_keys) : len(mixed_keys) + len(up_keys)]
    mixed_hbm, grad_hbm, rows_ref, grad_ref, mixed_sems, grad_sems = refs[len(mixed_keys) + len(up_keys) :]

    def source_place(dk, dz, dx):
        z = lax.bitwise_xor(seq // 8, dz)
        x = lax.bitwise_and(seq // 2 + dx, 3)
        k = lax.bitwise_xor(lax.bitwise_and(seq, 1), dk)
        return pl.ds(pl.multiple_of((z * 8 + x * 2 + k) * 32, 32), 32)

    places = [source_place(*key) for key in mixed_keys]
    sources = [ref.at[seq] for ref in mixed_refs]
    copies = fetch(sources, [mixed_hbm.at[place, :] for place in places], mixed_sems)
    total = lax.dot_general(
        whole_rows(mixed_refs), whole_rows(up_refs), (((1,), (1,)), ((), ())), preferred_element_type=F32
    )
    for i, place in enumerate(places):
        rows_ref[place, :] = total[32 * i : 32 * i + 32]
    turned_rows = rows_ref[...].T
    for i, (dy,) in enumerate(up_keys):
        for z in range(2):
            n = 2 * i + z
            place = pl.ds(pl.multiple_of((4 * z + lax.bitwise_and(chan + dy, 3)) * 32, 32), 32)
            grad_ref[32 * n : 32 * n + 32, :] = turned_rows[32 * n : 32 * n + 32]
            source = grad_ref.at[32 * n : 32 * n + 32, :]
            copies.append(pltpu.make_async_copy(source, grad_hbm.at[place, :], grad_sems.at[n]))
            copies[-1].start()
    for copy in copies:
        copy.wait()


def weight_gradient(mixed, up):
    mixed_keys, up_keys = [piece[1:] for piece in mixed], [piece[1:] for piece in up]
    return pl.pallas_call(
        functools.partial(grad_kernel, mixed_keys, up_keys),
        out_shape=(jax.ShapeDtypeStruct((512, 256), BF16), jax.ShapeDtypeStruct((256, 512), F32)),
        in_specs=vmem(len(mixed) + len(up)),
        out_specs=tuple(hbm(2)),
        scratch_shapes=[
            pltpu.VMEM((512, 256), F32),
            pltpu.VMEM((256, 512), F32),
            pltpu.SemaphoreType.DMA((len(mixed),)),
            pltpu.SemaphoreType.DMA((2 * len(up),)),
        ],
        cost_estimate=pl.CostEstimate(flops=1_000_000_000, bytes_accessed=7_000_000, transcendentals=0),
        compiler_params=limit(16),
        name="weight_gradient",
    )(*[piece[0] for piece in mixed], *[piece[0] for piece in up])


def exchange(value, axis):
    return lax.all_to_all(value, axis, split_axis=0, concat_axis=0, tiled=True)


def step(hidden_states, norm_gain, short_filter, long_filter, long_bias, gate_stream, upstream):
    consts = [jnp.asarray(table) for table in tables()]
    hidden, filt, gate = [value.reshape(16, 32, 256) for value in (hidden_states, long_filter, gate_stream)]
    payload, squares, lifted = pack(hidden, filt, upstream.reshape(16, 256, 256), norm_gain.reshape(4, INNER))
    squares = squares + over_chan(squares, 1, 0)
    got = exchange(payload, "seq")
    parts = [squares]
    for dy in (1, 3, 2):
        parts.append(over_chan(squares, 0, dy))
    payload = normalise(lifted, parts, gate)
    signal = exchange(payload, "seq")
    spec = filter_spectrum(got, short_filter, long_bias[None, :], consts)
    up = gather_chan(got[:, 32:96])
    mixed = gated_convolution(signal, spec, consts)
    return weight_gradient(gather_seq(mixed), up)


def solution(mesh):
    placed = (
        P("chan", "seq"),
        P("chan"),
        P("chan", None),
        P("chan", "seq"),
        P("chan"),
        P("chan", "seq"),
        P(None, "seq"),
    )
    return jax.shard_map(
        step,
        mesh=mesh,
        in_specs=placed,
        out_specs=(P("chan", "seq"), P("seq", "chan")),
        check_vma=False,
    )
```

```python
import functools
import math

import jax
import jax.numpy as jnp
import numpy as np
from jax import lax
from jax.experimental import pallas as pl
from jax.experimental.pallas import tpu as pltpu
from jax.sharding import PartitionSpec as P


D = 4096
EPSILON = 1e-05
OUTER = 32
INNER = 128
LENGTH = OUTER * INNER
BF16 = jnp.bfloat16
F32 = jnp.float32


def tables():
    m = np.arange(INNER, dtype=np.float64)
    turn = 2.0 * np.pi * (np.arange(OUTER)[:, None] + 0.25) * m[None, :] / LENGTH
    angle = 2.0 * np.pi * ((m[:, None] * m[None, :]) % INNER) / INNER
    cos, sin = np.cos(angle), np.sin(angle)
    ahead = np.block([[cos, -sin], [sin, cos]])
    back = np.block([[cos, sin], [-sin, cos]])
    parts = []
    for table in (ahead, back):
        upper = table.astype(BF16)
        lower = (table - upper.astype(np.float64)).astype(BF16)
        parts.append(np.concatenate([upper, lower]))
    return [np.stack([np.cos(turn), -np.sin(turn)]).astype(np.float32), np.stack(parts)]


def turned(value, step, total, sign):
    re, im = value
    step %= total
    if step == 0:
        return re, im
    if 4 * step == total:
        return (-im, re) if sign > 0 else (im, -re)
    half = math.sqrt(0.5)
    if 8 * step == total:
        return ((re - im) * half, (re + im) * half) if sign > 0 else ((re + im) * half, (im - re) * half)
    if 8 * step == 3 * total:
        if sign > 0:
            return (re + im) * -half, (re - im) * half
        return (im - re) * half, (re + im) * -half
    cos = math.cos(2.0 * math.pi * step / total)
    sin = sign * math.sin(2.0 * math.pi * step / total)
    return re * cos - im * sin, re * sin + im * cos


def transform(values, sign):
    total = len(values)
    if total == 1:
        return values
    even, odd = transform(values[0::2], sign), transform(values[1::2], sign)
    first, second = [], []
    for k in range(total // 2):
        er, ei = even[k]
        dr, di = turned(odd[k], k, total, sign)
        first.append((er + dr, ei + di))
        second.append((er - dr, ei - di))
    return first + second


def first_pass(load, half_ref, sign):
    for q in range(4):
        for k, value in enumerate(transform([load(4 * p + q) for p in range(8)], sign)):
            half_ref[q, k, 0], half_ref[q, k, 1] = turned(value, q * k, OUTER, sign)


def second_pass(store, half_ref, sign):
    for k in range(8):
        for j, value in enumerate(transform([(half_ref[q, k, 0], half_ref[q, k, 1]) for q in range(4)], sign)):
            store(k + 8 * j, value)


def row_groups():
    return [(g, slice(8 * g, 8 * g + 8)) for g in range(4)]


def outer_ahead(time_ref, mid_ref, half_ref, turn_ref, ready=None):
    for g, rows in row_groups():

        def load(n, rows=rows):
            x = time_ref[n, rows, :]
            angle = 2.0 * math.pi * n / (4 * OUTER)
            return x * math.cos(angle), x * -math.sin(angle)

        first_pass(load, half_ref.at[g], -1)
    if ready is not None:
        ready.wait()
    for g, rows in row_groups():

        def store(k, value, rows=rows):
            re, im = value
            tr, ti = turn_ref[0, k : k + 1, :], turn_ref[1, k : k + 1, :]
            mid_ref[k, rows, 0:INNER] = re * tr - im * ti
            mid_ref[k, rows, INNER:] = re * ti + im * tr

        second_pass(store, half_ref.at[g], -1)


def outer_back(mid_ref, time_ref, half_ref, turn_ref):
    for g, rows in row_groups():

        def load(k, rows=rows):
            re, im = mid_ref[k, rows, 0:INNER], mid_ref[k, rows, INNER:]
            tr, ti = turn_ref[0, k : k + 1, :], turn_ref[1, k : k + 1, :]
            return re * tr + im * ti, im * tr - re * ti

        def store(n, value, rows=rows):
            re, im = value
            angle = 2.0 * math.pi * n / (4 * OUTER)
            time_ref[n, rows, :] = re * (math.cos(angle) / LENGTH) - im * (math.sin(angle) / LENGTH)

        first_pass(load, half_ref.at[g], 1)
        second_pass(store, half_ref.at[g], 1)


def product(rows, table_ref):
    upper = rows.astype(BF16)
    lower = (rows - upper.astype(F32)).astype(BF16)
    dot = functools.partial(jnp.dot, preferred_element_type=F32)
    return dot(jnp.concatenate([upper, upper], axis=1), table_ref[...]) + dot(lower, table_ref[0 : 2 * INNER])


def complex_product(a, b):
    ar, ai, br, bi = a[:, :INNER], a[:, INNER:], b[:, :INNER], b[:, INNER:]
    return jnp.concatenate([ar * br - ai * bi, ar * bi + ai * br], axis=1)


CHUNK = 16


def chunks():
    return [slice(k, k + CHUNK) for k in range(0, OUTER, CHUNK)]


def flat(value):
    return value.reshape(value.shape[0] * value.shape[1], value.shape[2])


def column_of(row_ref, first):
    total = row_ref.shape[1]
    lane = lax.broadcasted_iota(jnp.int32, (32, total), 1)
    wanted = lax.broadcasted_iota(jnp.int32, (32, total), 0) + first
    return jnp.sum(jnp.where(lane == wanted, row_ref[...], 0.0), axis=1, keepdims=True)


def filter_kernel(
    got_ref,
    taps_hbm,
    bias_ref,
    turn_hbm,
    inner_hbm,
    spec_hbm,
    time_ref,
    mid_ref,
    half_ref,
    turn_ref,
    inner_ref,
    spec_ref,
    sems,
    spec_sems,
    taps_ref,
):
    first = pl.multiple_of(lax.axis_index("seq") * 32, 32)
    sources = (turn_hbm, taps_hbm.at[pl.ds(first, 32), :], inner_hbm)
    copies = fetch(sources, (turn_ref, taps_ref, inner_ref), sems)
    ahead, back = inner_ref.at[0], inner_ref.at[1]
    for b in range(16):
        for h in range(2):
            time_ref[2 * b + h] = got_ref[b, 0:32, h * INNER : (h + 1) * INNER].astype(F32)
    bias = column_of(bias_ref, first)
    lift = jnp.concatenate([jnp.broadcast_to(bias, (32, INNER)), jnp.zeros((32, INNER), F32)], axis=1)
    outer_ahead(time_ref, mid_ref, half_ref, turn_ref, copies[0])
    copies[1].wait()
    copies[2].wait()
    for ks in chunks():
        long = product(flat(mid_ref[ks]), ahead)
        long = long + jnp.tile(lift, (CHUNK, 1))
        taps = taps_ref[...][None]
        tr, ti = turn_ref[0, ks, :][:, None, :], turn_ref[1, ks, :][:, None, :]
        short = product(flat(jnp.concatenate([taps * tr, taps * ti], axis=2)), ahead)
        mid_ref[ks] = product(complex_product(long, short), back).reshape(CHUNK, 32, 2 * INNER)
    outer_back(mid_ref, time_ref, half_ref, turn_ref)
    outer_ahead(time_ref, mid_ref, half_ref, turn_ref)
    written = []
    for j, ks in enumerate(chunks()):
        spec_ref[ks] = product(flat(mid_ref[ks]), ahead).reshape(CHUNK, 32, 2 * INNER)
        written.append(pltpu.make_async_copy(spec_ref.at[ks], spec_hbm.at[ks], spec_sems.at[j]))
        written[-1].start()
    for copy in written:
        copy.wait()


def signal_kernel(
    got_ref,
    spec_hbm,
    turn_hbm,
    inner_hbm,
    mixed_ref,
    time_ref,
    mid_ref,
    half_ref,
    turn_ref,
    inner_ref,
    spec_ref,
    sems,
    spec_sems,
):
    copies = fetch((turn_hbm, inner_hbm), (turn_ref, inner_ref), sems)
    spec_copies = fetch([spec_hbm.at[ks] for ks in chunks()], [spec_ref.at[ks] for ks in chunks()], spec_sems)
    ahead, back = inner_ref.at[0], inner_ref.at[1]
    for b in range(16):
        for h in range(2):
            time_ref[2 * b + h] = got_ref[b, 0:32, h * INNER : (h + 1) * INNER].astype(F32)
    outer_ahead(time_ref, mid_ref, half_ref, turn_ref, copies[0])
    copies[1].wait()
    for ks, copy in zip(chunks(), spec_copies, strict=True):
        spec = product(flat(mid_ref[ks]), ahead)
        copy.wait()
        joint = complex_product(spec, flat(spec_ref[ks]))
        mid_ref[ks] = product(joint, back).reshape(CHUNK, 32, 2 * INNER)
    outer_back(mid_ref, time_ref, half_ref, turn_ref)
    for b in range(16):
        for h in range(2):
            cols = slice(h * INNER, (h + 1) * INNER)
            long_out = time_ref[2 * b + h].astype(BF16).astype(F32)
            mixed_ref[b, :, cols] = (got_ref[b, 32:64, cols].astype(F32) * long_out).astype(BF16)


def vmem(count):
    return [pl.BlockSpec(memory_space=pltpu.VMEM)] * count


def hbm(count):
    return [pl.BlockSpec(memory_space=pltpu.HBM)] * count


def stay(value):
    return pltpu.with_memory_space_constraint(value, pltpu.HBM)


def fetch(sources, targets, sems):
    copies = [pltpu.make_async_copy(source, target, sems.at[i]) for i, (source, target) in enumerate(zip(sources, targets))]
    for copy in copies:
        copy.start()
    return copies


SCRATCH = [
    pltpu.VMEM((OUTER, 32, INNER), F32),
    pltpu.VMEM((OUTER, 32, 2 * INNER), F32),
    pltpu.VMEM((4, 4, 8, 2, 8, INNER), F32),
    pltpu.VMEM((2, OUTER, INNER), F32),
    pltpu.VMEM((2, 4 * INNER, 2 * INNER), BF16),
    pltpu.VMEM((OUTER, 32, 2 * INNER), F32),
    pltpu.SemaphoreType.DMA((3,)),
    pltpu.SemaphoreType.DMA((OUTER // CHUNK,)),
]


def filter_spectrum(got, taps, bias, consts):
    return pl.pallas_call(
        filter_kernel,
        out_shape=pltpu.HBM((OUTER, 32, 2 * INNER), F32),
        in_specs=[*vmem(1), *hbm(1), *vmem(1), *hbm(2)],
        out_specs=hbm(1)[0],
        scratch_shapes=[*SCRATCH, pltpu.VMEM((32, INNER), F32)],
        cost_estimate=pl.CostEstimate(flops=2_000_000_000, bytes_accessed=3_000_000, transcendentals=0),
        compiler_params=limit(8),
        name="filter_spectrum",
    )(got, stay(taps), bias, *[stay(value) for value in consts])


def gated_convolution(got, spec, consts):
    return pl.pallas_call(
        signal_kernel,
        out_shape=jax.ShapeDtypeStruct((16, 32, 256), BF16),
        in_specs=vmem(1) + hbm(3),
        out_specs=vmem(1)[0],
        scratch_shapes=SCRATCH,
        cost_estimate=pl.CostEstimate(flops=1_000_000_000, bytes_accessed=3_000_000, transcendentals=0),
        compiler_params=limit(8),
    )(got, stay(spec), *[stay(value) for value in consts])


def pack_kernel(
    hidden_hbm, long_ref, up_ref, gain_hbm, payload_hbm, squares_ref, lifted_ref, hidden, gain_ref, held, sems, out_sems
):
    chan = lax.axis_index("chan")
    pair = [pl.ds(pl.multiple_of((lax.bitwise_and(chan, 3) + 4 * z) * 32, 32), 32) for z in range(2)]
    sources = [gain_hbm, hidden_hbm, long_ref, up_ref.at[:, pair[0], :], up_ref.at[:, pair[1], :]]
    targets = [gain_ref, hidden, *[held.at[i] for i in range(3)]]
    copies = fetch(sources, targets, sems)
    copies[0].wait()
    gains = [jnp.broadcast_to(gain_ref[q : q + 1, :], (INNER, INNER)).T for q in range(4)]
    leaving = []
    for i in range(3):
        copies[2 + i].wait()
        leaving.append(
            pltpu.make_async_copy(held.at[i], payload_hbm.at[:, 32 * i : 32 * i + 32, :], out_sems.at[i])
        )
        leaving[-1].start()
    copies[1].wait()
    total = jnp.zeros((8, 256), F32)
    for b in range(16):
        states = hidden[b].astype(F32)
        powers = states * states
        for r in range(4):
            total = total + powers[8 * r : 8 * r + 8]
        gain = gains[b // 4][32 * (b % 4) : 32 * (b % 4) + 32]
        lifted_ref[b] = states * jnp.concatenate([gain, gain], axis=1)
    squares_ref[...] = total
    for copy in leaving:
        copy.wait()


def norm_kernel(lifted_ref, s0, s1, s2, s3, gate_hbm, payload_ref, sems):
    (copy,) = fetch([gate_hbm], [payload_ref.at[:, 32:64, :]], sems)
    squares = (s0[...] + s1[...]) + (s2[...] + s3[...])
    scale = lax.rsqrt(jnp.sum(squares, axis=0, keepdims=True) / D + EPSILON)
    for b in range(16):
        payload_ref[b, 0:32, :] = (lifted_ref[b] * scale).astype(BF16)
    copy.wait()


def limit(mib):
    return pltpu.CompilerParams(vmem_limit_bytes=mib * 2**20)


def pack(hidden, long_filter, upstream, gain):
    return pl.pallas_call(
        pack_kernel,
        out_shape=(
            jax.ShapeDtypeStruct((16, 96, 256), BF16),
            jax.ShapeDtypeStruct((8, 256), F32),
            jax.ShapeDtypeStruct((16, 32, 256), F32),
        ),
        in_specs=hbm(4),
        out_specs=(*hbm(1), *vmem(2)),
        scratch_shapes=[
            pltpu.VMEM((16, 32, 256), BF16),
            pltpu.VMEM((4, INNER), F32),
            pltpu.VMEM((3, 16, 32, 256), BF16),
            pltpu.SemaphoreType.DMA((5,)),
            pltpu.SemaphoreType.DMA((3,)),
        ],
        compiler_params=limit(6),
        name="pack",
    )(stay(hidden), stay(long_filter), stay(upstream), stay(gain))


def normalise(lifted, squares, gate):
    return pl.pallas_call(
        norm_kernel,
        out_shape=jax.ShapeDtypeStruct((16, 64, 256), BF16),
        in_specs=vmem(5) + hbm(1),
        out_specs=vmem(1)[0],
        scratch_shapes=[pltpu.SemaphoreType.DMA((1,))],
        compiler_params=limit(6),
        name="normalise",
    )(lifted, *squares, stay(gate))


def place_of(s):
    return s // 8, (s // 2) % 4, s % 2


def over_seq(value, dz, dx, dk):
    pairs = []
    for s in range(16):
        z, x, k = place_of(s)
        pairs.append((s, (z ^ dz) * 8 + ((x + dx) % 4) * 2 + (k ^ dk)))
    return lax.ppermute(value, "seq", pairs)


def over_chan(value, dz, dy):
    pairs = [(c, ((c // 4) ^ dz) * 4 + (c + dy) % 4) for c in range(8)]
    return lax.ppermute(value, "chan", pairs)


def gather_seq(own):
    side = over_seq(own, 1, 0, 0)
    near = {(0, 0): own, (1, 0): side}
    for dx in (3, 1, 2):
        near[0, dx] = over_seq(own, 0, -dx, 0)
    for dx in (3, 1):
        near[1, dx] = over_seq(side, 0, -dx, 0)
    near[1, 2] = over_seq(near[0, 2], 1, 0, 0)
    pieces = []
    for (dz, dx), value in near.items():
        pieces += [(value, 0, dz, dx), (over_seq(value, 0, 0, 1), 1, dz, dx)]
    return pieces


def gather_chan(own):
    pieces = [(own, 0)]
    for dy in (3, 1, 2):
        pieces.append((over_chan(own, 0, -dy), dy))
    return pieces


def whole_rows(refs):
    return jnp.concatenate([jnp.concatenate([ref[b] for b in range(16)], axis=1) for ref in refs], axis=0)


def grad_kernel(mixed_keys, up_keys, *refs):
    seq, chan = lax.axis_index("seq"), lax.axis_index("chan")
    mixed_refs, up_refs = refs[: len(mixed_keys)], refs[len(mixed_keys) : len(mixed_keys) + len(up_keys)]
    mixed_hbm, grad_ref, rows_ref, mixed_sems = refs[len(mixed_keys) + len(up_keys) :]

    def source_place(dk, dz, dx):
        z = lax.bitwise_xor(seq // 8, dz)
        x = lax.bitwise_and(seq // 2 + dx, 3)
        k = lax.bitwise_xor(lax.bitwise_and(seq, 1), dk)
        return pl.ds(pl.multiple_of((z * 8 + x * 2 + k) * 32, 32), 32)

    places = [source_place(*key) for key in mixed_keys]
    sources = [ref.at[seq] for ref in mixed_refs]
    copies = fetch(sources, [mixed_hbm.at[place, :] for place in places], mixed_sems)
    total = lax.dot_general(
        whole_rows(mixed_refs), whole_rows(up_refs), (((1,), (1,)), ((), ())), preferred_element_type=F32
    )
    for i, place in enumerate(places):
        rows_ref[place, :] = total[32 * i : 32 * i + 32]
    turned_rows = rows_ref[...].T
    for i, (dy,) in enumerate(up_keys):
        for z in range(2):
            n = 2 * i + z
            place = pl.ds(pl.multiple_of((4 * z + lax.bitwise_and(chan + dy, 3)) * 32, 32), 32)
            grad_ref[place, :] = turned_rows[32 * n : 32 * n + 32]
    for copy in copies:
        copy.wait()


def weight_gradient(mixed, up):
    mixed_keys, up_keys = [piece[1:] for piece in mixed], [piece[1:] for piece in up]
    return pl.pallas_call(
        functools.partial(grad_kernel, mixed_keys, up_keys),
        out_shape=(jax.ShapeDtypeStruct((512, 256), BF16), jax.ShapeDtypeStruct((256, 512), F32)),
        in_specs=vmem(len(mixed) + len(up)),
        out_specs=(*hbm(1), *vmem(1)),
        scratch_shapes=[
            pltpu.VMEM((512, 256), F32),
            pltpu.SemaphoreType.DMA((len(mixed),)),
        ],
        cost_estimate=pl.CostEstimate(flops=1_000_000_000, bytes_accessed=7_000_000, transcendentals=0),
        compiler_params=limit(16),
        name="weight_gradient",
    )(*[piece[0] for piece in mixed], *[piece[0] for piece in up])


def exchange(value, axis):
    return lax.all_to_all(value, axis, split_axis=0, concat_axis=0, tiled=True)


def step(hidden_states, norm_gain, short_filter, long_filter, long_bias, gate_stream, upstream):
    consts = [jnp.asarray(table) for table in tables()]
    hidden, filt, gate = [value.reshape(16, 32, 256) for value in (hidden_states, long_filter, gate_stream)]
    payload, squares, lifted = pack(hidden, filt, upstream.reshape(16, 256, 256), norm_gain.reshape(4, INNER))
    squares = squares + over_chan(squares, 1, 0)
    got = exchange(payload, "seq")
    parts = [squares]
    for dy in (1, 3, 2):
        parts.append(over_chan(squares, 0, dy))
    payload = normalise(lifted, parts, gate)
    signal = exchange(payload, "seq")
    spec = filter_spectrum(got, short_filter, long_bias[None, :], consts)
    up = gather_chan(got[:, 32:96])
    mixed = gated_convolution(signal, spec, consts)
    return weight_gradient(gather_seq(mixed), up)


def solution(mesh):
    placed = (
        P("chan", "seq"),
        P("chan"),
        P("chan", None),
        P("chan", "seq"),
        P("chan"),
        P("chan", "seq"),
        P(None, "seq"),
    )
    return jax.shard_map(
        step,
        mesh=mesh,
        in_specs=placed,
        out_specs=(P("chan", "seq"), P("seq", "chan")),
        check_vma=False,
    )
```
